256 devices in a mesh: seq: 64 (over y, z, core), batch: 4 (over x).
Axes of the slice: x: 4, y: 4, z: 8, core: 2. Of those that a mesh axis runs over, the one named last changes fastest.
Arguments:
- queries: bfloat16 [65536, 256], P(('batch', 'seq')), parts along dimension 0, may hold values from -0.5 to 0.5
- keys: bfloat16 [65536, 256], P(('batch', 'seq')), parts along dimension 0, may hold values from -0.5 to 0.5
- values: bfloat16 [65536, 512], P(('batch', 'seq')), parts along dimension 0, may hold values from -6 to 6
- log_decay: float32 [65536, 256], P(('batch', 'seq')), parts along dimension 0, may hold values from -1 to 0, as said below
- out_grad: bfloat16 [65536, 512], P(('batch', 'seq')), parts along dimension 0, may hold values from -0.19921875 to 0.19921875
Outputs:
- grad_queries: bfloat16 [65536, 256], P(('batch', 'seq')), parts along dimension 0
- grad_keys: bfloat16 [65536, 256], P(('batch', 'seq')), parts along dimension 0
- grad_values: bfloat16 [65536, 512], P(('batch', 'seq')), parts along dimension 0
- grad_decay: float32 [65536, 256], P(('batch', 'seq')), parts along dimension 0
The draws below stay inside these ranges and needn't reach their ends.
There are 4 independent parts, one for each index of `batch`. The reference program is written for one: setup_inputs(seed, part) draws one part's arguments, and reference() takes and returns one part's arrays. A program takes and returns all parts, laid end to end along the dimension named above; each array names one. Nothing has to cross between parts.
Inputs may be any that keep to these rules, and one draw needn't show every extreme that they name: `log_decay`: log of a decay factor per position and key channel.
All inputs are finite; a program needn't handle non-finite values.
Results may differ from the reference program's by a relative error of at most 0.001.
Values sent between devices are 32-bit elements; how exact they have to be, the bound alone decides.
No kernel may reach another device: no remote copies, remote signals or barrier semaphores. Data moves between devices by JAX's collectives and lax.ppermute only.
A program may use at most 128 MiB of HBM per device.

```python
import jax
import jax.numpy as jnp
from jax import lax

H = 2
K = 128
V = 256
GROUP = 64
TOK_DEV = 256
LENGTH = 16384
N_SEQ = 64


def draw_log_decay(key, part):
    sequence_extent = TOK_DEV * N_SEQ
    hidden_dimension = H * K
    number_of_streams = jax.random.split(jax.random.fold_in(key, 17), 7)
    fast_share = 0.5
    fast = jax.random.bernoulli(number_of_streams[0], fast_share, (hidden_dimension,))
    span = jax.random.uniform(number_of_streams[1], (hidden_dimension,), jnp.float32, 30.0, 50.0)
    slow_scale = jax.random.uniform(number_of_streams[2], (hidden_dimension,), jnp.float32, 0.03, 0.15)
    base = jnp.where(fast, jnp.log(10.0) / span, slow_scale * jnp.log(10.0) / sequence_extent)
    device_factor = jnp.exp(jax.random.uniform(number_of_streams[3], (N_SEQ, 1, hidden_dimension), jnp.float32, -0.69, 0.69))
    rough = jax.random.uniform(number_of_streams[4], (N_SEQ, TOK_DEV, hidden_dimension), jnp.float32, 0.5, 1.5)
    incoming_frequency = (base[None, None, :] * device_factor * rough).reshape(sequence_extent, hidden_dimension)
    places = jax.random.randint(number_of_streams[5], (2,), 0, sequence_extent)
    number_of_hits = jnp.any(jnp.arange(sequence_extent)[:, None] == places[None, :], axis=1)
    packet_quantity = jnp.log(jax.random.uniform(number_of_streams[6], (sequence_extent, hidden_dimension), jnp.float32, 0.5, 0.8))
    return (-incoming_frequency + jnp.where(number_of_hits[:, None], packet_quantity, 0.0)).astype(jnp.float32)


def levels(stream_key, extent, shards, low, largest):
    factor_of, own = 1.0, jax.random.fold_in(stream_key, 6)
    for position, blocks in shards:
        draws = jnp.exp(jax.random.uniform(jax.random.fold_in(own, position), (blocks,), jnp.float32, low / len(shards), largest / len(shards)))
        factor_of = factor_of * jnp.repeat(draws, extent[position] // blocks).reshape([-1 if axis == position else 1 for axis in range(len(extent))])
    return factor_of


def normal_values(key, dims, spread, bound, cuts=(), held_as=jnp.bfloat16):
    level = levels(key, dims, cuts, -0.22, 0.18) if cuts else 1.0
    result = jax.random.normal(key, dims, jnp.float32) * spread * level
    return jnp.minimum(jnp.maximum(result, -bound), bound).astype(held_as)


def setup_inputs(seed: int = 0, part: int = 0) -> dict:
    key_of = jax.random.split(jax.random.key(seed), 6)
    part_splits = jax.random.split(jax.random.fold_in(key_of[5], part), 6)
    queries = normal_values(part_splits[0], (LENGTH, H * K), K ** -0.5, 0.5, ((0, 64),))
    keys = normal_values(part_splits[1], (LENGTH, H * K), K ** -0.5, 0.5, ((0, 64),))
    values = normal_values(part_splits[2], (LENGTH, H * V), 1.0, 6.0, ((0, 64),))
    log_decay = draw_log_decay(jax.random.fold_in(jax.random.fold_in(key_of[5], part), 71), part)
    out_grad = normal_values(part_splits[4], (LENGTH, H * V), 0.03125, 0.19921875, ((0, 64),))
    return dict(queries=queries, keys=keys, values=values, log_decay=log_decay, out_grad=out_grad)


HIGHEST_PRECISION = lax.Precision.HIGHEST


def outer_product(form, left, right):
    return jnp.einsum(form, left, right, precision=HIGHEST_PRECISION, preferred_element_type=jnp.float32)


def reference(queries, keys, values, log_decay, out_grad):
    sequence_extent = queries.shape[0]
    blocks = sequence_extent // GROUP
    query_rows = queries.astype(jnp.float32).reshape(blocks, GROUP, H, K)
    key_rows = keys.astype(jnp.float32).reshape(blocks, GROUP, H, K)
    value_rows = values.astype(jnp.float32).reshape(blocks, GROUP, H, V)
    grad_rows = out_grad.astype(jnp.float32).reshape(blocks, GROUP, H, V)
    within = jnp.cumsum(log_decay.reshape(blocks, GROUP, H, K), axis=1)
    block_sum = within[:, -1]
    rising = jnp.exp(within)
    falling = jnp.exp(-within)
    tail_gate = jnp.exp(block_sum[:, None] - within)
    q_gate = query_rows * rising
    k_gate = key_rows * falling
    k_tail = key_rows * tail_gate
    causal = jnp.tril(jnp.ones((GROUP, GROUP), jnp.float32))
    zero_state = jnp.zeros((H, K, V), jnp.float32)

    def forward_step(carried_state, inputs):
        kg_block, lookup_final_slab, value_tile, gradient_tile, rise_block, summed_decay = inputs
        pair_dots = outer_product('thv,shv->hts', gradient_tile, value_tile) * causal
        grad_q = rise_block * (outer_product('hts,shk->thk', pair_dots, kg_block)
                               + outer_product('pzn,zyn->pzy', gradient_tile, carried_state))
        carried_state = jnp.exp(summed_decay)[..., None] * carried_state + outer_product('mln,mls->lns', lookup_final_slab, value_tile)
        return carried_state, grad_q

    unused_end, grad_q = lax.scan(forward_step, zero_state,
                                  (k_gate, k_tail, value_rows, grad_rows, rising, block_sum))

    def backward_step(carried_gradient, inputs):
        query_gate_tile, kg_block, lookup_final_slab, value_tile, gradient_tile, fall_block, trailing_tile, summed_decay = inputs
        score_matrix = outer_product('thk,shk->hts', query_gate_tile, kg_block) * causal
        pair_dots = outer_product('thv,shv->hts', gradient_tile, value_tile) * causal
        grad_k = fall_block * outer_product('hts,thk->shk', pair_dots, query_gate_tile) \
            + trailing_tile * outer_product('bdz,dlz->bdl', value_tile, carried_gradient)
        value_gradient = outer_product('nbj,bne->jne', score_matrix, gradient_tile) + outer_product('icd,cda->ica', lookup_final_slab, carried_gradient)
        carried_gradient = outer_product('mln,mls->lns', query_gate_tile, gradient_tile) + jnp.exp(summed_decay)[..., None] * carried_gradient
        return carried_gradient, (grad_k, value_gradient)

    unused_start, (grad_k, value_gradient) = lax.scan(
        backward_step, zero_state,
        (q_gate, k_gate, k_tail, value_rows, grad_rows, falling, tail_gate, block_sum), reverse=True)
    dg_terms = (query_rows * grad_q - key_rows * grad_k).reshape(sequence_extent, H * K)
    grad_decay = lax.cumsum(dg_terms, axis=0, reverse=True)
    return (grad_q.reshape(sequence_extent, H * K).astype(jnp.bfloat16),
            grad_k.reshape(sequence_extent, H * K).astype(jnp.bfloat16),
            value_gradient.reshape(sequence_extent, H * V).astype(jnp.bfloat16),
            grad_decay)
```

```python
import jax
import jax.numpy as jnp
from jax import lax
from jax.experimental import pallas as pl
from jax.experimental.pallas import tpu as pltpu
from jax.sharding import Mesh
from jax.sharding import PartitionSpec as P

H = 2
K = 128
V = 256
GROUP = 64
TOK = 256
HK = H * K
Y, Z, CORES = 4, 8, 2
CHIPS = Y * Z
ROWS = V // CHIPS
MSG = ROWS + 1
CHIP_AXES = ("seq_y", "seq_z")
SPEC = P(("batch", "seq_y", "seq_z", "seq_c"), None)
F32 = jnp.float32
BF16 = jnp.bfloat16


def dot(left, right, dims):
    return lax.dot_general(left, right, (dims, ((), ())), preferred_element_type=F32)


def nn(left, right):
    return dot(left, right, ((1,), (0,)))


def nt(left, right):
    return dot(left, right, ((1,), (1,)))


def tn(left, right):
    return dot(left, right, ((0,), (0,)))


def split(x):
    hi = x.astype(BF16)
    return hi, (x - hi.astype(F32)).astype(BF16)


def split3(x):
    hi = x.astype(BF16)
    rest = x - hi.astype(F32)
    mid = rest.astype(BF16)
    return hi, mid, (rest - mid.astype(F32)).astype(BF16)


def summed(x, suffix):
    rows = x.shape[0]
    r = lax.broadcasted_iota(jnp.int32, (rows, rows), 0)
    c = lax.broadcasted_iota(jnp.int32, (rows, rows), 1)
    ones = jnp.where((c >= r) if suffix else (c <= r), 1.0, 0.0).astype(BF16)
    hi, mid, lo = split3(x)
    return nn(ones, hi) + (nn(ones, mid) + nn(ones, lo))


def head(h, width):
    return slice(h * width, (h + 1) * width)


def folded(out):
    half = out.shape[1] // 2
    return out[:, :half] + out[:, half:]


def ends_kernel(q_ref, k_ref, v_ref, do_ref, g_ref, send_ref, e_ref, f_ref, b_ref):
    first = lax.axis_index("seq_c") == 0
    b = summed(g_ref[...], False)
    b_ref[...] = b
    total = b[TOK - 1 :]
    k_tail = k_ref[...].astype(F32) * jnp.exp(total - b)
    q_gate = q_ref[...].astype(F32) * jnp.exp(b)
    for h in range(H):
        hk, hv = head(h, K), head(h, V)
        e_ref[:, hk] = folded(tn(v_ref[:, hv], jnp.concatenate(split(k_tail[:, hk]), 1)))
        f_ref[:, hk] = folded(tn(do_ref[:, hv], jnp.concatenate(split(q_gate[:, hk]), 1)))

    @pl.when(first)
    def _():
        send_ref[:V] = f_ref[...]

    @pl.when(jnp.logical_not(first))
    def _():
        send_ref[:V] = e_ref[...]

    send_ref[V:] = jnp.broadcast_to(total, (8, HK))


def message_kernel(e_ref, f_ref, b_ref, got_ref, msg_ref):
    first = lax.axis_index("seq_c") == 0
    total = b_ref[TOK - 1 :]
    other = got_ref[V : V + 1]
    gate = jnp.exp(other)
    chip_gate = jnp.exp(total + other)

    def write(kept_ref):
        for i in range(CHIPS):
            rows = slice(i * ROWS, (i + 1) * ROWS)
            msg_ref[i * MSG : i * MSG + ROWS, 0, :] = kept_ref[rows] * gate + got_ref[rows]
            msg_ref[i * MSG + ROWS] = chip_gate

    @pl.when(first)
    def _():
        write(e_ref)

    @pl.when(jnp.logical_not(first))
    def _():
        write(f_ref)


def scan_kernel(msg_ref, out_ref):
    first = lax.axis_index("seq_c") == 0
    state = jnp.zeros((ROWS, HK), F32)
    for i in range(CHIPS):
        at = jnp.where(first, i, CHIPS - 1 - i)
        out_ref[pl.ds(pl.multiple_of(at * ROWS, ROWS), ROWS)] = state
        state = msg_ref[at * MSG + ROWS] * state + msg_ref[pl.ds(at * MSG, ROWS), 0, :]


def onward_kernel(e_ref, f_ref, b_ref, came_ref, send_ref):
    first = lax.axis_index("seq_c") == 0
    gate = jnp.exp(b_ref[TOK - 1 :])

    @pl.when(first)
    def _():
        send_ref[...] = gate * came_ref[...] + e_ref[...]

    @pl.when(jnp.logical_not(first))
    def _():
        send_ref[...] = gate * came_ref[...] + f_ref[...]


def inner_kernel(q_ref, k_ref, v_ref, do_ref, b_ref, dq_ref, dk_ref, dv_ref):
    r = lax.broadcasted_iota(jnp.int32, (TOK, TOK), 0)
    c = lax.broadcasted_iota(jnp.int32, (TOK, TOK), 1)
    for h in range(H):
        hk, hv = head(h, K), head(h, V)
        q = q_ref[:, hk].astype(F32)
        k = k_ref[:, hk].astype(F32)
        b = b_ref[:, hk]
        pair = jnp.where(c <= r, nt(do_ref[:, hv], v_ref[:, hv]), 0.0)
        pair_t = jnp.where(c >= r, nt(v_ref[:, hv], do_ref[:, hv]), 0.0)
        p_hi, p_lo = split(pair)
        t_hi, t_lo = split(pair_t)
        dk = jnp.zeros((TOK, K), F32)
        dv = jnp.zeros((TOK, V), F32)
        for i in range(TOK // GROUP):
            rows = slice(i * GROUP, (i + 1) * GROUP)
            end = (i + 1) * GROUP
            upto = slice(0, end)
            start = b[i * GROUP - 1 : i * GROUP] if i else jnp.zeros((1, K), F32)
            rising = jnp.exp(b[rows] - start)
            falling = jnp.exp(start - b[upto])
            q_hi, q_lo = split(q[rows] * rising)
            k_hi, k_lo = split(k[upto] * falling)
            scores_t = nt(k_hi, q_hi) + (nt(k_hi, q_lo) + nt(k_lo, q_hi))
            rr = lax.broadcasted_iota(jnp.int32, (end, GROUP), 0)
            cc = lax.broadcasted_iota(jnp.int32, (end, GROUP), 1) + i * GROUP
            s_hi, s_lo = split(jnp.where(cc >= rr, scores_t, 0.0))
            k_both = jnp.concatenate((k_hi, k_lo), 1)
            q_both = jnp.concatenate((q_hi, q_lo), 1)
            dq_ref[rows, hk] = rising * (
                folded(nn(p_hi[rows, upto], k_both)) + nn(p_lo[rows, upto], k_hi)
            )
            dk_part = falling * (folded(nn(t_hi[upto, rows], q_both)) + nn(t_lo[upto, rows], q_hi))
            dv_part = nn(s_hi, do_ref[rows, hv]) + nn(s_lo, do_ref[rows, hv])
            if end < TOK:
                dk_part = jnp.concatenate((dk_part, jnp.zeros((TOK - end, K), F32)), 0)
                dv_part = jnp.concatenate((dv_part, jnp.zeros((TOK - end, V), F32)), 0)
            dk = dk + dk_part
            dv = dv + dv_part
        dk_ref[:, hk] = dk
        dv_ref[:, hv] = dv


def grads_kernel(
    q_ref, k_ref, v_ref, do_ref, b_ref, e_ref, came_ref, got_ref, dqi_ref, dki_ref, dvi_ref,
    dq_ref, dk_ref, dv_ref, dg_ref, s_ref, g_ref,
):
    first = lax.axis_index("seq_c") == 0

    @pl.when(first)
    def _():
        s_ref[...] = came_ref[...]
        g_ref[...] = got_ref[...]

    @pl.when(jnp.logical_not(first))
    def _():
        s_ref[...] = got_ref[...]
        g_ref[...] = came_ref[...]

    for h in range(H):
        hk, hv = head(h, K), head(h, V)
        q = q_ref[:, hk].astype(F32)
        k = k_ref[:, hk].astype(F32)
        b = b_ref[:, hk]
        total = b[TOK - 1 :]
        rising = jnp.exp(b)
        tail = jnp.exp(total - b)
        state = s_ref[:, hk]
        grad = g_ref[:, hk]
        g_hi, g_lo = split(grad)
        dq = dqi_ref[:, hk] + rising * folded(
            nn(do_ref[:, hv], jnp.concatenate(split(state), 1))
        )
        dk = dki_ref[:, hk] + tail * folded(
            nn(v_ref[:, hv], jnp.concatenate((g_hi, g_lo), 1))
        )
        t_hi, t_lo = split(k * tail)
        dv = dvi_ref[:, hv] + (nt(t_hi, g_hi) + (nt(t_lo, g_hi) + nt(t_hi, g_lo)))
        dq_ref[:, hk] = dq.astype(BF16)
        dk_ref[:, hk] = dk.astype(BF16)
        dv_ref[:, hv] = dv.astype(BF16)
        end_state = jnp.exp(total) * state + e_ref[:, hk]
        later = jnp.sum(end_state * grad, axis=0, keepdims=True)
        dg_ref[:, hk] = summed(q * dq - k * dk, True) + later


def call(kernel, outs, *args, scratch=(), flops=1000000):
    whole = pl.BlockSpec(memory_space=pltpu.VMEM)
    shapes = [jax.ShapeDtypeStruct(shape, dtype) for shape, dtype in outs]
    out = pl.pallas_call(
        kernel,
        out_shape=shapes,
        in_specs=[whole] * len(args),
        out_specs=[whole] * len(outs),
        scratch_shapes=list(scratch),
        cost_estimate=pl.CostEstimate(flops=flops, bytes_accessed=2000000, transcendentals=0),
        compiler_params=pltpu.CompilerParams(vmem_limit_bytes=32 << 20),
    )(*args)
    return out if len(outs) > 1 else out[0]


SWAP = [(0, 1), (1, 0)]
SQUARE = ((TOK, HK), F32)


def local(q, k, v, log_decay, do):
    send, e, f, b = call(
        ends_kernel, [((V + 8, HK), F32), SQUARE, SQUARE, SQUARE], q, k, v, do, log_decay
    )
    got = lax.ppermute(send, "seq_c", SWAP)
    msg = call(message_kernel, [((CHIPS * MSG, 1, HK), F32)], e, f, b, got)
    msg = lax.all_to_all(msg, CHIP_AXES, 0, 0, tiled=True)
    back = call(scan_kernel, [SQUARE], msg)
    came = lax.all_to_all(
        back.reshape(CHIPS, ROWS, HK), CHIP_AXES, 0, 0, tiled=True
    ).reshape(V, HK)
    onward = call(onward_kernel, [SQUARE], e, f, b, came)
    got = lax.ppermute(onward, "seq_c", SWAP)
    inner = call(
        inner_kernel, [SQUARE, SQUARE, ((TOK, H * V), F32)], q, k, v, do, b, flops=200000000
    )
    return call(
        grads_kernel,
        [((TOK, HK), BF16), ((TOK, HK), BF16), ((TOK, H * V), BF16), SQUARE],
        q, k, v, do, b, e, came, got, *inner,
        scratch=[pltpu.VMEM((V, HK), F32)] * 2,
    )


def solution(mesh):
    finer = Mesh(
        mesh.devices.reshape(Y, Z, CORES, mesh.shape["batch"]),
        ("seq_y", "seq_z", "seq_c", "batch"),
    )
    return jax.shard_map(
        local, mesh=finer, in_specs=(SPEC,) * 5, out_specs=(SPEC,) * 4, check_vma=False
    )
```

```python
import jax
import jax.numpy as jnp
from jax import lax
from jax.experimental import pallas as pl
from jax.experimental.pallas import tpu as pltpu
from jax.sharding import Mesh
from jax.sharding import PartitionSpec as P

H = 2
K = 128
V = 256
GROUP = 64
TOK = 256
HK = H * K
HV = H * V
Y, Z, CORES = 4, 8, 2
CHIPS = Y * Z
ROWS = V // CHIPS
MSG = ROWS + 1
CHIP_AXES = ("seq_y", "seq_z")
SPEC = P(("batch", "seq_y", "seq_z", "seq_c"), None)
F32 = jnp.float32
BF16 = jnp.bfloat16


def dot(left, right, dims):
    return lax.dot_general(left, right, (dims, ((), ())), preferred_element_type=F32)


def nn(left, right):
    return dot(left, right, ((1,), (0,)))


def nt(left, right):
    return dot(left, right, ((1,), (1,)))


def tn(left, right):
    return dot(left, right, ((0,), (0,)))


def split(x):
    hi = x.astype(BF16)
    return hi, (x - hi.astype(F32)).astype(BF16)


def pair(x):
    return jnp.concatenate(split(x), 1)


def folded(out):
    half = out.shape[1] // 2
    return out[:, :half] + out[:, half:]


def running_sum(x):
    rows = x.shape[0]
    r = lax.broadcasted_iota(jnp.int32, (rows, rows), 0)
    c = lax.broadcasted_iota(jnp.int32, (rows, rows), 1)
    ones = jnp.where(c <= r, 1.0, 0.0).astype(BF16)
    hi = x.astype(BF16)
    rest = x - hi.astype(F32)
    mid, lo = split(rest)
    return nn(ones, hi) + (nn(ones, mid) + nn(ones, lo))


def head(h, width):
    return slice(h * width, (h + 1) * width)


def at_head(h, width):
    return pl.ds(pl.multiple_of(h * width, width), width)


def halves(left, right):
    return jnp.concatenate((left, right), 1)


def block_ends(q_ref, k_ref, v_ref, do_ref, b_ref, out_ref, h):
    hk, hv = at_head(h, K), at_head(h, V)
    b = b_ref[:, hk]
    total = b_ref[TOK - 1 :, hk]
    out_ref[:V, :K] = folded(tn(v_ref[:, hv], pair(k_ref[:, hk].astype(F32) * jnp.exp(total - b))))
    out_ref[:V, K:] = folded(tn(do_ref[:, hv], pair(q_ref[:, hk].astype(F32) * jnp.exp(b))))


def first_kernel(
    q_hbm, k_hbm, v_hbm, do_hbm, g_hbm, q_ref, k_ref, v_ref, do_ref, b_ref, send_ref, g_ref, sems
):
    copies = [
        pltpu.make_async_copy(source, target, sems.at[n])
        for n, (source, target) in enumerate(
            ((g_hbm, g_ref), (k_hbm, k_ref), (v_hbm, v_ref), (q_hbm, q_ref), (do_hbm, do_ref))
        )
    ]
    for copy in copies:
        copy.start()
    copies[0].wait()
    b_ref[...] = running_sum(g_ref[...])
    for copy in copies[1:]:
        copy.wait()
    h = 1 - lax.axis_index("seq_c")
    block_ends(q_ref, k_ref, v_ref, do_ref, b_ref, send_ref, h)
    total = b_ref[TOK - 1 :, at_head(h, K)]
    send_ref[V:] = jnp.broadcast_to(halves(total, total), (8, HK))


def second_kernel(q_ref, k_ref, v_ref, do_ref, b_ref, own_ref):
    block_ends(q_ref, k_ref, v_ref, do_ref, b_ref, own_ref, lax.axis_index("seq_c"))


def lane_gates(b_ref, got_ref):
    core = lax.axis_index("seq_c")
    total = b_ref[TOK - 1 :, at_head(core, K)]
    mine = jnp.exp(halves(total, total))
    other = jnp.exp(got_ref[V : V + 1])
    forward = lax.broadcasted_iota(jnp.int32, (1, HK), 1) < K
    return mine, other, forward, core == 0


def pick(flag, forward, when_true, when_false):
    return jnp.where(jnp.logical_xor(forward, jnp.logical_not(flag)), when_true, when_false)


def message_kernel(own_ref, got_ref, b_ref, msg_ref, token_ref):
    mine, other, forward, first = lane_gates(b_ref, got_ref)
    own_gate = pick(first, forward, other, 1.0)
    got_gate = pick(first, forward, 1.0, mine)
    both = mine * other
    for i in range(CHIPS):
        rows = slice(i * ROWS, (i + 1) * ROWS)
        msg_ref[i * MSG : i * MSG + ROWS, 0, :] = own_ref[rows] * own_gate + got_ref[rows] * got_gate
        msg_ref[i * MSG + ROWS] = both
    token_ref[...] = jnp.zeros_like(token_ref)


def scan_kernel(msg_ref, _, out_ref):
    for order, lanes in ((range(CHIPS), slice(0, K)), (range(CHIPS - 1, -1, -1), slice(K, HK))):
        state = jnp.zeros((ROWS, K), F32)
        for i in order:
            out_ref[i * ROWS : (i + 1) * ROWS, lanes] = state
            gate = msg_ref[i * MSG + ROWS, :, lanes]
            state = gate * state + msg_ref[i * MSG : i * MSG + ROWS, 0, lanes]


def onward_kernel(own_ref, got_ref, b_ref, came_ref, send_ref, mine_ref):
    mine, other, forward, first = lane_gates(b_ref, got_ref)
    came = came_ref[...]
    send_ref[...] = came * pick(first, forward, mine, 1.0) + pick(
        first, forward, own_ref[...], 0.0
    )
    mine_ref[...] = came * pick(first, forward, 1.0, other) + pick(
        first, forward, 0.0, got_ref[:V]
    )


def inner_kernel(
    q_ref, k_ref, v_ref, do_ref, b_ref, _,
    dq_ref, dk_ref, dv_ref, rise_ref, tail_ref, kt_hi_ref, kt_lo_ref, token_ref,
):
    r = lax.broadcasted_iota(jnp.int32, (TOK, TOK), 0)
    c = lax.broadcasted_iota(jnp.int32, (TOK, TOK), 1)
    for h in range(H):
        hk, hv = head(h, K), head(h, V)
        q = q_ref[:, hk].astype(F32)
        k = k_ref[:, hk].astype(F32)
        b = b_ref[:, hk]
        dots = jnp.where(c <= r, nt(do_ref[:, hv], v_ref[:, hv]), 0.0)
        dots_t = jnp.where(c >= r, nt(v_ref[:, hv], do_ref[:, hv]), 0.0)
        p_hi, p_lo = split(dots)
        t_hi, t_lo = split(dots_t)
        dk = jnp.zeros((TOK, K), F32)
        dv = jnp.zeros((TOK, V), F32)
        for i in range(TOK // GROUP):
            rows = slice(i * GROUP, (i + 1) * GROUP)
            end = (i + 1) * GROUP
            upto = slice(0, end)
            start = b[i * GROUP - 1 : i * GROUP] if i else jnp.zeros((1, K), F32)
            rising = jnp.exp(b[rows] - start)
            falling = jnp.exp(start - b[upto])
            q_hi, q_lo = split(q[rows] * rising)
            k_hi, k_lo = split(k[upto] * falling)
            scores_t = nt(k_hi, q_hi) + (nt(k_hi, q_lo) + nt(k_lo, q_hi))
            rr = lax.broadcasted_iota(jnp.int32, (end, GROUP), 0)
            cc = lax.broadcasted_iota(jnp.int32, (end, GROUP), 1) + i * GROUP
            s_hi, s_lo = split(jnp.where(cc >= rr, scores_t, 0.0))
            k_both = halves(k_hi, k_lo)
            q_both = halves(q_hi, q_lo)
            dq_ref[rows, hk] = rising * (
                folded(nn(p_hi[rows, upto], k_both)) + nn(p_lo[rows, upto], k_hi)
            )
            dk_part = falling * (folded(nn(t_hi[upto, rows], q_both)) + nn(t_lo[upto, rows], q_hi))
            dv_part = nn(s_hi, do_ref[rows, hv]) + nn(s_lo, do_ref[rows, hv])
            if end < TOK:
                dk_part = jnp.concatenate((dk_part, jnp.zeros((TOK - end, K), F32)), 0)
                dv_part = jnp.concatenate((dv_part, jnp.zeros((TOK - end, V), F32)), 0)
            dk = dk + dk_part
            dv = dv + dv_part
        dk_ref[:, hk] = dk
        dv_ref[:, hv] = dv
        tail = jnp.exp(b[TOK - 1 :] - b)
        rise_ref[:, hk] = jnp.exp(b)
        tail_ref[:, hk] = tail
        kt_hi_ref[:, hk], kt_lo_ref[:, hk] = split(k * tail)
    token_ref[...] = jnp.zeros_like(token_ref)


def grads_kernel(
    own, q_ref, k_ref, v_ref, do_ref, b_ref, end_ref, in_ref, dqi_ref, dki_ref, dvi_ref,
    rise_ref, tail_ref, kt_hi_ref, kt_lo_ref, *rest,
):
    dq_hbm, dk_hbm, dv_hbm, dg_hbm, dq_ref, dk_ref, dv_ref, dg_ref, sems = rest[-9:]
    core = lax.axis_index("seq_c")
    h = core if own else 1 - core
    hk, hv = at_head(h, K), at_head(h, V)
    outs = ((dq_ref, dq_hbm, hk), (dk_ref, dk_hbm, hk), (dv_ref, dv_hbm, hv), (dg_ref, dg_hbm, hk))
    dq_out, dk_out, dv_out, dg_out = (
        pltpu.make_async_copy(source, target.at[:, lanes], sems.at[n])
        for n, (source, target, lanes) in enumerate(outs)
    )
    state = in_ref[:, :K]
    grad = in_ref[:, K:]
    g_hi, g_lo = split(grad)
    dq = dqi_ref[:, hk] + rise_ref[:, hk] * folded(nn(do_ref[:, hv], pair(state)))
    dk = dki_ref[:, hk] + tail_ref[:, hk] * folded(nn(v_ref[:, hv], halves(g_hi, g_lo)))
    dq_ref[...] = dq.astype(BF16)
    dq_out.start()
    dk_ref[...] = dk.astype(BF16)
    dk_out.start()
    t_hi, t_lo = kt_hi_ref[:, hk], kt_lo_ref[:, hk]
    dv = dvi_ref[:, hv] + (nt(halves(t_hi, t_lo), halves(g_hi, g_hi)) + nt(t_hi, g_lo))
    dv_ref[...] = dv.astype(BF16)
    dv_out.start()
    end_state = jnp.exp(b_ref[TOK - 1 :, hk]) * state + end_ref[:V, :K]
    later = jnp.sum(end_state * grad, axis=0, keepdims=True)
    terms = q_ref[:, hk].astype(F32) * dq - k_ref[:, hk].astype(F32) * dk
    r = lax.broadcasted_iota(jnp.int32, (TOK, TOK), 0)
    c = lax.broadcasted_iota(jnp.int32, (TOK, TOK), 1)
    ones = jnp.where(c >= r, 1.0, 0.0).astype(BF16)
    dg_ref[...] = folded(nn(ones, pair(terms))) + later
    dg_out.start()
    for copy in (dq_out, dk_out, dv_out, dg_out):
        copy.wait()


VMEM = pl.BlockSpec(memory_space=pltpu.VMEM)
HBM = pl.BlockSpec(memory_space=pltpu.HBM)
SQUARE = ((TOK, HK), F32)
SQUARE16 = ((TOK, HK), BF16)
WIDE16 = ((TOK, HV), BF16)
TOKEN = ((8, 128), F32)


def call(kernel, outs, *args, specs=None, out_specs=None, scratch=(), flops=1000000, alias=None):
    shapes = [jax.ShapeDtypeStruct(shape, dtype) for shape, dtype in outs]
    out = pl.pallas_call(
        kernel,
        out_shape=shapes,
        in_specs=specs or [VMEM] * len(args),
        out_specs=out_specs or [VMEM] * len(outs),
        scratch_shapes=list(scratch),
        input_output_aliases=alias or {},
        cost_estimate=pl.CostEstimate(flops=flops, bytes_accessed=2000000, transcendentals=0),
        compiler_params=pltpu.CompilerParams(vmem_limit_bytes=32 << 20),
    )(*args)
    return out if len(outs) > 1 else out[0]


SWAP = [(0, 1), (1, 0)]
GRAD_OUTS = [SQUARE16, SQUARE16, WIDE16, SQUARE]
GRAD_SCRATCH = [
    pltpu.VMEM((TOK, K), BF16),
    pltpu.VMEM((TOK, K), BF16),
    pltpu.VMEM((TOK, V), BF16),
    pltpu.VMEM((TOK, K), F32),
    pltpu.SemaphoreType.DMA((4,)),
]


def grads(own, args, into=()):
    def kernel(*refs):
        grads_kernel(own, *refs)

    return call(
        kernel,
        GRAD_OUTS,
        *args,
        *into,
        specs=[VMEM] * len(args) + [HBM] * len(into),
        out_specs=[HBM] * 4,
        scratch=GRAD_SCRATCH,
        flops=100000000,
        alias={len(args) + n: n for n in range(len(into))},
    )


def local(q, k, v, log_decay, do):
    q, k, v, do, log_decay = (pltpu.with_memory_space_constraint(x, pltpu.HBM) for x in (q, k, v, do, log_decay))
    q, k, v, do, b, send = call(
        first_kernel,
        [SQUARE16, SQUARE16, WIDE16, WIDE16, SQUARE, ((V + 8, HK), F32)],
        q, k, v, do, log_decay,
        specs=[HBM] * 5,
        scratch=[pltpu.VMEM((TOK, HK), F32), pltpu.SemaphoreType.DMA((5,))],
    )
    got = lax.ppermute(send, "seq_c", SWAP)
    own = call(second_kernel, [((V, HK), F32)], q, k, v, do, b, flops=100000000)
    msg, token = call(message_kernel, [((CHIPS * MSG, 1, HK), F32), TOKEN], own, got, b)
    msg = lax.all_to_all(msg, CHIP_AXES, 0, 0, tiled=True)
    *inner, token = call(
        inner_kernel,
        [SQUARE, SQUARE, ((TOK, HV), F32), SQUARE, SQUARE, SQUARE16, SQUARE16, TOKEN],
        q, k, v, do, b, token,
        flops=20000000000,
    )
    back = call(scan_kernel, [SQUARE], msg, token)
    came = lax.all_to_all(
        back.reshape(CHIPS, ROWS, HK), CHIP_AXES, 0, 0, tiled=True
    ).reshape(V, HK)
    onward, mine = call(onward_kernel, [SQUARE, SQUARE], own, got, b, came)
    theirs = lax.ppermute(onward, "seq_c", SWAP)
    half = grads(True, (q, k, v, do, b, own, mine, *inner))
    return grads(False, (q, k, v, do, b, send, theirs, *inner), half)


def solution(mesh):
    finer = Mesh(
        mesh.devices.reshape(Y, Z, CORES, mesh.shape["batch"]),
        ("seq_y", "seq_z", "seq_c", "batch"),
    )
    return jax.shard_map(
        local, mesh=finer, in_specs=(SPEC,) * 5, out_specs=(SPEC,) * 4, check_vma=False
    )
```

```python
import jax
import jax.numpy as jnp
from jax import lax
from jax.experimental import pallas as pl
from jax.experimental.pallas import tpu as pltpu
from jax.sharding import Mesh
from jax.sharding import PartitionSpec as P

H = 2
K = 128
V = 256
GROUP = 64
TOK = 256
HK = H * K
HV = H * V
Y, Z, CORES = 4, 8, 2
CHIPS = Y * Z
ROWS = V // CHIPS
MSG = ROWS + 1
CHIP_AXES = ("seq_y", "seq_z")
SPEC = P(("batch", "seq_y", "seq_z", "seq_c"), None)
F32 = jnp.float32
BF16 = jnp.bfloat16


def dot(left, right, dims):
    return lax.dot_general(left, right, (dims, ((), ())), preferred_element_type=F32)


def nn(left, right):
    return dot(left, right, ((1,), (0,)))


def nt(left, right):
    return dot(left, right, ((1,), (1,)))


def tn(left, right):
    return dot(left, right, ((0,), (0,)))


def split(x):
    hi = x.astype(BF16)
    return hi, (x - hi.astype(F32)).astype(BF16)


def pair(x):
    return jnp.concatenate(split(x), 1)


def folded(out):
    half = out.shape[1] // 2
    return out[:, :half] + out[:, half:]


def running_sum(x):
    rows = x.shape[0]
    r = lax.broadcasted_iota(jnp.int32, (rows, rows), 0)
    c = lax.broadcasted_iota(jnp.int32, (rows, rows), 1)
    ones = jnp.where(c <= r, 1.0, 0.0).astype(BF16)
    hi = x.astype(BF16)
    rest = x - hi.astype(F32)
    mid, lo = split(rest)
    return nn(ones, hi) + (nn(ones, mid) + nn(ones, lo))


def head(h, width):
    return slice(h * width, (h + 1) * width)


def at_head(h, width):
    return pl.ds(pl.multiple_of(h * width, width), width)


def halves(left, right):
    return jnp.concatenate((left, right), 1)


def block_ends(q_ref, k_ref, v_ref, do_ref, b_ref, out_ref, h):
    hk, hv = at_head(h, K), at_head(h, V)
    b = b_ref[:, hk]
    total = b_ref[TOK - 1 :, hk]
    out_ref[:V, :K] = folded(tn(v_ref[:, hv], pair(k_ref[:, hk].astype(F32) * jnp.exp(total - b))))
    out_ref[:V, K:] = folded(tn(do_ref[:, hv], pair(q_ref[:, hk].astype(F32) * jnp.exp(b))))


def first_kernel(
    q_hbm, k_hbm, v_hbm, do_hbm, g_hbm, q_ref, k_ref, v_ref, do_ref, b_ref, send_ref, g_ref, sems
):
    copies = [
        pltpu.make_async_copy(source, target, sems.at[n])
        for n, (source, target) in enumerate(
            ((g_hbm, g_ref), (k_hbm, k_ref), (v_hbm, v_ref), (q_hbm, q_ref), (do_hbm, do_ref))
        )
    ]
    for copy in copies:
        copy.start()
    copies[0].wait()
    b_ref[...] = running_sum(g_ref[...])
    for copy in copies[1:]:
        copy.wait()
    h = 1 - lax.axis_index("seq_c")
    block_ends(q_ref, k_ref, v_ref, do_ref, b_ref, send_ref, h)
    total = b_ref[TOK - 1 :, at_head(h, K)]
    send_ref[V:] = jnp.broadcast_to(halves(total, total), (8, HK))


def inner_pairs(q_ref, k_ref, v_ref, do_ref, b_ref, h, dq_ref, dk_ref, dv_ref):
    hk, hv = at_head(h, K), at_head(h, V)
    r = lax.broadcasted_iota(jnp.int32, (TOK, TOK), 0)
    c = lax.broadcasted_iota(jnp.int32, (TOK, TOK), 1)
    q = q_ref[:, hk].astype(F32)
    k = k_ref[:, hk].astype(F32)
    b = b_ref[:, hk]
    v = v_ref[:, hv]
    do = do_ref[:, hv]
    p_hi, p_lo = split(jnp.where(c <= r, nt(do, v), 0.0))
    t_hi, t_lo = split(jnp.where(c >= r, nt(v, do), 0.0))
    dk = jnp.zeros((TOK, K), F32)
    dv = jnp.zeros((TOK, V), F32)
    for i in range(TOK // GROUP):
        rows = slice(i * GROUP, (i + 1) * GROUP)
        end = (i + 1) * GROUP
        upto = slice(0, end)
        start = b[i * GROUP - 1 : i * GROUP] if i else jnp.zeros((1, K), F32)
        rising = jnp.exp(b[rows] - start)
        falling = jnp.exp(start - b[upto])
        q_hi, q_lo = split(q[rows] * rising)
        k_hi, k_lo = split(k[upto] * falling)
        scores_t = nt(k_hi, q_hi) + (nt(k_hi, q_lo) + nt(k_lo, q_hi))
        rr = lax.broadcasted_iota(jnp.int32, (end, GROUP), 0)
        cc = lax.broadcasted_iota(jnp.int32, (end, GROUP), 1) + i * GROUP
        s_hi, s_lo = split(jnp.where(cc >= rr, scores_t, 0.0))
        dq_ref[rows] = rising * (
            folded(nn(p_hi[rows, upto], halves(k_hi, k_lo))) + nn(p_lo[rows, upto], k_hi)
        )
        dk_part = falling * (
            folded(nn(t_hi[upto, rows], halves(q_hi, q_lo))) + nn(t_lo[upto, rows], q_hi)
        )
        dv_part = nn(s_hi, do[rows]) + nn(s_lo, do[rows])
        if end < TOK:
            dk_part = jnp.concatenate((dk_part, jnp.zeros((TOK - end, K), F32)), 0)
            dv_part = jnp.concatenate((dv_part, jnp.zeros((TOK - end, V), F32)), 0)
        dk = dk + dk_part
        dv = dv + dv_part
    dk_ref[...] = dk
    dv_ref[...] = dv


def outer_gates(k_ref, b_ref, h, rise_ref, tail_ref, kt_ref):
    hk = at_head(h, K)
    b = b_ref[:, hk]
    tail = jnp.exp(b_ref[TOK - 1 :, hk] - b)
    rise_ref[...] = jnp.exp(b)
    tail_ref[...] = tail
    kt_ref[...] = pair(k_ref[:, hk].astype(F32) * tail)


def second_kernel(q_ref, k_ref, v_ref, do_ref, b_ref, own_ref, *inner_refs):
    core = lax.axis_index("seq_c")
    block_ends(q_ref, k_ref, v_ref, do_ref, b_ref, own_ref, core)
    outer_gates(k_ref, b_ref, core, *inner_refs[3:])
    inner_pairs(q_ref, k_ref, v_ref, do_ref, b_ref, core, *inner_refs[:3])


def lane_gates(b_ref, got_ref):
    core = lax.axis_index("seq_c")
    total = b_ref[TOK - 1 :, at_head(core, K)]
    mine = jnp.exp(halves(total, total))
    other = jnp.exp(got_ref[V : V + 1])
    forward = lax.broadcasted_iota(jnp.int32, (1, HK), 1) < K
    return mine, other, forward, core == 0


def pick(flag, forward, when_true, when_false):
    return jnp.where(jnp.logical_xor(forward, jnp.logical_not(flag)), when_true, when_false)


def message_kernel(own_ref, got_ref, b_ref, msg_ref):
    mine, other, forward, first = lane_gates(b_ref, got_ref)
    own_gate = pick(first, forward, other, 1.0)
    got_gate = pick(first, forward, 1.0, mine)
    both = mine * other
    for i in range(CHIPS):
        rows = slice(i * ROWS, (i + 1) * ROWS)
        msg_ref[i * MSG : i * MSG + ROWS, 0, :] = own_ref[rows] * own_gate + got_ref[rows] * got_gate
        msg_ref[i * MSG + ROWS] = both


def scan_kernel(msg_ref, out_ref):
    for order, lanes in ((range(CHIPS), slice(0, K)), (range(CHIPS - 1, -1, -1), slice(K, HK))):
        state = jnp.zeros((ROWS, K), F32)
        for i in order:
            out_ref[i * ROWS : (i + 1) * ROWS, lanes] = state
            gate = msg_ref[i * MSG + ROWS, :, lanes]
            state = gate * state + msg_ref[i * MSG : i * MSG + ROWS, 0, lanes]


def onward_kernel(own_ref, got_ref, b_ref, came_ref, send_ref, mine_ref):
    mine, other, forward, first = lane_gates(b_ref, got_ref)
    came = came_ref[...]
    send_ref[...] = came * pick(first, forward, mine, 1.0) + pick(
        first, forward, own_ref[...], 0.0
    )
    mine_ref[...] = came * pick(first, forward, 1.0, other) + pick(
        first, forward, 0.0, got_ref[:V]
    )


def head_grads(
    h, q_ref, k_ref, v_ref, do_ref, b_ref, end_ref, in_ref,
    dqi_ref, dki_ref, dvi_ref, rise_ref, tail_ref, kt_ref, dq_ref, dk_ref, dv_ref, dg_ref, stored,
):
    hk, hv = at_head(h, K), at_head(h, V)
    state = in_ref[:, :K]
    grad = in_ref[:, K:]
    g_hi, g_lo = split(grad)
    dq = dqi_ref[...] + rise_ref[...] * folded(nn(do_ref[:, hv], pair(state)))
    dk = dki_ref[...] + tail_ref[...] * folded(nn(v_ref[:, hv], halves(g_hi, g_lo)))
    dq_ref[...] = dq.astype(BF16)
    stored(0)
    dk_ref[...] = dk.astype(BF16)
    stored(1)
    dv = dvi_ref[...] + (nt(kt_ref[...], halves(g_hi, g_hi)) + nt(kt_ref[:, :K], g_lo))
    dv_ref[...] = dv.astype(BF16)
    stored(2)
    end_state = jnp.exp(b_ref[TOK - 1 :, hk]) * state + end_ref[:V, :K]
    later = jnp.sum(end_state * grad, axis=0, keepdims=True)
    terms = q_ref[:, hk].astype(F32) * dq - k_ref[:, hk].astype(F32) * dk
    r = lax.broadcasted_iota(jnp.int32, (TOK, TOK), 0)
    c = lax.broadcasted_iota(jnp.int32, (TOK, TOK), 1)
    ones = jnp.where(c >= r, 1.0, 0.0).astype(BF16)
    dg_ref[...] = folded(nn(ones, pair(terms))) + later
    stored(3)


def own_grads_kernel(q_ref, k_ref, v_ref, do_ref, b_ref, own_ref, in_ref, *rest):
    core = lax.axis_index("seq_c")
    args = (q_ref, k_ref, v_ref, do_ref, b_ref)
    head_grads(core, *args, own_ref, in_ref, *rest[:6], *rest[6:10], lambda n: None)
    outer_gates(k_ref, b_ref, 1 - core, *rest[13:])
    inner_pairs(*args, 1 - core, *rest[10:13])


def final_kernel(q_ref, k_ref, v_ref, do_ref, b_ref, sent_ref, in_ref, *rest):
    inner_refs, mine, outs, theirs, sems = rest[:6], rest[6:10], rest[10:14], rest[14:18], rest[18]
    core = lax.axis_index("seq_c")
    widths = (K, K, V, K)

    def copies(sources, h, base):
        return [
            pltpu.make_async_copy(source, out.at[:, at_head(h, width)], sems.at[base + n])
            for n, (source, out, width) in enumerate(zip(sources, outs, widths))
        ]

    first = copies(mine, core, 0)
    second = copies(theirs, 1 - core, 4)
    for copy in first:
        copy.start()
    head_grads(
        1 - core, q_ref, k_ref, v_ref, do_ref, b_ref, sent_ref, in_ref, *inner_refs, *theirs,
        lambda n: second[n].start(),
    )
    for copy in first + second:
        copy.wait()


VMEM = pl.BlockSpec(memory_space=pltpu.VMEM)
HBM = pl.BlockSpec(memory_space=pltpu.HBM)
SQUARE = ((TOK, HK), F32)
SQUARE16 = ((TOK, HK), BF16)
WIDE16 = ((TOK, HV), BF16)
HALF = ((TOK, K), F32)
INNER = [HALF, HALF, ((TOK, V), F32), HALF, HALF, ((TOK, 2 * K), BF16)]
HALF_GRADS = [((TOK, K), BF16), ((TOK, K), BF16), ((TOK, V), BF16), HALF]


def call(kernel, outs, *args, specs=None, out_specs=None, scratch=(), flops=1000000):
    shapes = [jax.ShapeDtypeStruct(shape, dtype) for shape, dtype in outs]
    out = pl.pallas_call(
        kernel,
        out_shape=shapes,
        in_specs=specs or [VMEM] * len(args),
        out_specs=out_specs or [VMEM] * len(outs),
        scratch_shapes=list(scratch),
        cost_estimate=pl.CostEstimate(flops=flops, bytes_accessed=2000000, transcendentals=0),
        compiler_params=pltpu.CompilerParams(vmem_limit_bytes=32 << 20),
    )(*args)
    return out if len(outs) > 1 else out[0]


SWAP = [(0, 1), (1, 0)]


def local(q, k, v, log_decay, do):
    q, k, v, do, log_decay = (
        pltpu.with_memory_space_constraint(x, pltpu.HBM) for x in (q, k, v, do, log_decay)
    )
    q, k, v, do, b, send = call(
        first_kernel,
        [SQUARE16, SQUARE16, WIDE16, WIDE16, SQUARE, ((V + 8, HK), F32)],
        q, k, v, do, log_decay,
        specs=[HBM] * 5,
        scratch=[pltpu.VMEM((TOK, HK), F32), pltpu.SemaphoreType.DMA((5,))],
    )
    got = lax.ppermute(send, "seq_c", SWAP)
    own, *inner = call(second_kernel, [SQUARE, *INNER], q, k, v, do, b, flops=100000000)
    msg = call(message_kernel, [((CHIPS * MSG, 1, HK), F32)], own, got, b)
    msg = lax.all_to_all(msg, CHIP_AXES, 0, 0, tiled=True)
    back = call(scan_kernel, [SQUARE], msg)
    came = lax.all_to_all(
        back.reshape(CHIPS, ROWS, HK), CHIP_AXES, 0, 0, tiled=True
    ).reshape(V, HK)
    onward, mine = call(onward_kernel, [SQUARE, SQUARE], own, got, b, came)
    theirs = lax.ppermute(onward, "seq_c", SWAP)
    done = call(
        own_grads_kernel,
        HALF_GRADS + INNER,
        q, k, v, do, b, own, mine, *inner,
        flops=100000000,
    )
    return call(
        final_kernel,
        [SQUARE16, SQUARE16, WIDE16, SQUARE],
        q, k, v, do, b, send, theirs, *done[4:], *done[:4],
        out_specs=[HBM] * 4,
        scratch=[pltpu.VMEM(*out) for out in HALF_GRADS] + [pltpu.SemaphoreType.DMA((8,))],
    )


def solution(mesh):
    finer = Mesh(
        mesh.devices.reshape(Y, Z, CORES, mesh.shape["batch"]),
        ("seq_y", "seq_z", "seq_c", "batch"),
    )
    return jax.shard_map(
        local, mesh=finer, in_specs=(SPEC,) * 5, out_specs=(SPEC,) * 4, check_vma=False
    )
```

```python
import jax
import jax.numpy as jnp
from jax import lax
from jax.experimental import pallas as pl
from jax.experimental.pallas import tpu as pltpu
from jax.sharding import PartitionSpec as P

H = 2
K = 128
V = 256
GROUP = 64
TOK = 256
HK = H * K
HV = H * V
Y, Z, CORES = 4, 8, 2
CHIPS = Y * Z
ROWS = V // CHIPS
MSG = ROWS + 1
SPEC = P(("batch", "seq"), None)
FIRST = (Y // 2, Z // 2)
LISTED = [((y + FIRST[0]) % Y) * Z + (z + FIRST[1]) % Z for y in range(Y) for z in range(Z)]
GROUPS = [[CORES * chip + core for chip in LISTED] for core in range(CORES)]
SWAP = [(device, device ^ 1) for device in range(CHIPS * CORES)]
F32 = jnp.float32
BF16 = jnp.bfloat16


def core_index():
    return lax.rem(lax.axis_index("seq"), CORES)


def exchanged(x):
    return lax.all_to_all(x, "seq", 0, 0, axis_index_groups=GROUPS, tiled=True)


def dot(left, right, dims):
    return lax.dot_general(left, right, (dims, ((), ())), preferred_element_type=F32)


def nn(left, right):
    return dot(left, right, ((1,), (0,)))


def nt(left, right):
    return dot(left, right, ((1,), (1,)))


def tn(left, right):
    return dot(left, right, ((0,), (0,)))


def split(x):
    hi = x.astype(BF16)
    return hi, (x - hi.astype(F32)).astype(BF16)


def pair(x):
    return jnp.concatenate(split(x), 1)


def folded(out):
    half = out.shape[1] // 2
    return out[:, :half] + out[:, half:]


def running_sum(x):
    rows = x.shape[0]
    r = lax.broadcasted_iota(jnp.int32, (rows, rows), 0)
    c = lax.broadcasted_iota(jnp.int32, (rows, rows), 1)
    ones = jnp.where(c <= r, 1.0, 0.0).astype(BF16)
    hi = x.astype(BF16)
    rest = x - hi.astype(F32)
    mid, lo = split(rest)
    return nn(ones, hi) + (nn(ones, mid) + nn(ones, lo))


def head(h, width):
    return slice(h * width, (h + 1) * width)


def at_head(h, width):
    return pl.ds(pl.multiple_of(h * width, width), width)


def halves(left, right):
    return jnp.concatenate((left, right), 1)


def block_ends(q_ref, k_ref, v_ref, do_ref, b_ref, out_ref, h):
    hk, hv = at_head(h, K), at_head(h, V)
    b = b_ref[:, hk]
    total = b_ref[TOK - 1 :, hk]
    out_ref[:V, :K] = folded(tn(v_ref[:, hv], pair(k_ref[:, hk].astype(F32) * jnp.exp(total - b))))
    out_ref[:V, K:] = folded(tn(do_ref[:, hv], pair(q_ref[:, hk].astype(F32) * jnp.exp(b))))


def first_kernel(
    q_hbm, k_hbm, v_hbm, do_hbm, g_hbm, q_ref, k_ref, v_ref, do_ref, b_ref, send_ref, g_ref, sems
):
    copies = [
        pltpu.make_async_copy(source, target, sems.at[n])
        for n, (source, target) in enumerate(
            ((g_hbm, g_ref), (k_hbm, k_ref), (v_hbm, v_ref), (q_hbm, q_ref), (do_hbm, do_ref))
        )
    ]
    for copy in copies:
        copy.start()
    copies[0].wait()
    b_ref[...] = running_sum(g_ref[...])
    for copy in copies[1:]:
        copy.wait()
    h = 1 - core_index()
    block_ends(q_ref, k_ref, v_ref, do_ref, b_ref, send_ref, h)
    total = b_ref[TOK - 1 :, at_head(h, K)]
    send_ref[V:] = jnp.broadcast_to(halves(total, total), (8, HK))


def inner_pairs(q_ref, k_ref, v_ref, do_ref, b_ref, h, dq_ref, dk_ref, dv_ref):
    hk, hv = at_head(h, K), at_head(h, V)
    r = lax.broadcasted_iota(jnp.int32, (TOK, TOK), 0)
    c = lax.broadcasted_iota(jnp.int32, (TOK, TOK), 1)
    q = q_ref[:, hk].astype(F32)
    k = k_ref[:, hk].astype(F32)
    b = b_ref[:, hk]
    v = v_ref[:, hv]
    do = do_ref[:, hv]
    p_hi, p_lo = split(jnp.where(c <= r, nt(do, v), 0.0))
    t_hi, t_lo = split(jnp.where(c >= r, nt(v, do), 0.0))
    dk = jnp.zeros((TOK, K), F32)
    dv = jnp.zeros((TOK, V), F32)
    for i in range(TOK // GROUP):
        rows = slice(i * GROUP, (i + 1) * GROUP)
        end = (i + 1) * GROUP
        upto = slice(0, end)
        start = b[i * GROUP - 1 : i * GROUP] if i else jnp.zeros((1, K), F32)
        rising = jnp.exp(b[rows] - start)
        falling = jnp.exp(start - b[upto])
        q_hi, q_lo = split(q[rows] * rising)
        k_hi, k_lo = split(k[upto] * falling)
        scores_t = nt(k_hi, q_hi) + (nt(k_hi, q_lo) + nt(k_lo, q_hi))
        rr = lax.broadcasted_iota(jnp.int32, (end, GROUP), 0)
        cc = lax.broadcasted_iota(jnp.int32, (end, GROUP), 1) + i * GROUP
        s_hi, s_lo = split(jnp.where(cc >= rr, scores_t, 0.0))
        dq_ref[rows] = rising * (
            folded(nn(p_hi[rows, upto], halves(k_hi, k_lo))) + nn(p_lo[rows, upto], k_hi)
        )
        dk_part = falling * (
            folded(nn(t_hi[upto, rows], halves(q_hi, q_lo))) + nn(t_lo[upto, rows], q_hi)
        )
        dv_part = nn(s_hi, do[rows]) + nn(s_lo, do[rows])
        if end < TOK:
            dk_part = jnp.concatenate((dk_part, jnp.zeros((TOK - end, K), F32)), 0)
            dv_part = jnp.concatenate((dv_part, jnp.zeros((TOK - end, V), F32)), 0)
        dk = dk + dk_part
        dv = dv + dv_part
    dk_ref[...] = dk
    dv_ref[...] = dv


def outer_gates(k_ref, b_ref, h, rise_ref, tail_ref, kt_ref):
    hk = at_head(h, K)
    b = b_ref[:, hk]
    tail = jnp.exp(b_ref[TOK - 1 :, hk] - b)
    rise_ref[...] = jnp.exp(b)
    tail_ref[...] = tail
    kt_ref[...] = pair(k_ref[:, hk].astype(F32) * tail)


def second_kernel(q_ref, k_ref, v_ref, do_ref, b_ref, own_ref, *inner_refs):
    core = core_index()
    block_ends(q_ref, k_ref, v_ref, do_ref, b_ref, own_ref, core)
    outer_gates(k_ref, b_ref, core, *inner_refs[3:])
    inner_pairs(q_ref, k_ref, v_ref, do_ref, b_ref, core, *inner_refs[:3])


def lane_gates(b_ref, got_ref):
    core = core_index()
    total = b_ref[TOK - 1 :, at_head(core, K)]
    mine = jnp.exp(halves(total, total))
    other = jnp.exp(got_ref[V : V + 1])
    forward = lax.broadcasted_iota(jnp.int32, (1, HK), 1) < K
    return mine, other, forward, core == 0


def pick(flag, forward, when_true, when_false):
    return jnp.where(jnp.logical_xor(forward, jnp.logical_not(flag)), when_true, when_false)


def message_kernel(own_ref, got_ref, b_ref, msg_ref):
    mine, other, forward, first = lane_gates(b_ref, got_ref)
    own_gate = pick(first, forward, other, 1.0)
    got_gate = pick(first, forward, 1.0, mine)
    both = mine * other
    for i in range(CHIPS):
        rows = slice(i * ROWS, (i + 1) * ROWS)
        msg_ref[i * MSG : i * MSG + ROWS, 0, :] = own_ref[rows] * own_gate + got_ref[rows] * got_gate
        msg_ref[i * MSG + ROWS] = both


def scan_kernel(msg_ref, out_ref):
    places = [LISTED.index(chip) for chip in range(CHIPS)]
    for order, lanes in ((places, slice(0, K)), (places[::-1], slice(K, HK))):
        state = jnp.zeros((ROWS, K), F32)
        for i in order:
            out_ref[i * ROWS : (i + 1) * ROWS, lanes] = state
            gate = msg_ref[i * MSG + ROWS, :, lanes]
            state = gate * state + msg_ref[i * MSG : i * MSG + ROWS, 0, lanes]


def onward_kernel(own_ref, got_ref, b_ref, came_ref, send_ref, mine_ref):
    mine, other, forward, first = lane_gates(b_ref, got_ref)
    came = came_ref[...]
    send_ref[...] = came * pick(first, forward, mine, 1.0) + pick(
        first, forward, own_ref[...], 0.0
    )
    mine_ref[...] = came * pick(first, forward, 1.0, other) + pick(
        first, forward, 0.0, got_ref[:V]
    )


def head_grads(
    h, q_ref, k_ref, v_ref, do_ref, b_ref, end_ref, in_ref,
    dqi_ref, dki_ref, dvi_ref, rise_ref, tail_ref, kt_ref, dq_ref, dk_ref, dv_ref, dg_ref, stored,
):
    hk, hv = at_head(h, K), at_head(h, V)
    state = in_ref[:, :K]
    grad = in_ref[:, K:]
    g_hi, g_lo = split(grad)
    dq = dqi_ref[...] + rise_ref[...] * folded(nn(do_ref[:, hv], pair(state)))
    dk = dki_ref[...] + tail_ref[...] * folded(nn(v_ref[:, hv], halves(g_hi, g_lo)))
    dq_ref[...] = dq.astype(BF16)
    stored(0)
    dk_ref[...] = dk.astype(BF16)
    stored(1)
    dv = dvi_ref[...] + (nt(kt_ref[...], halves(g_hi, g_hi)) + nt(kt_ref[:, :K], g_lo))
    dv_ref[...] = dv.astype(BF16)
    stored(2)
    end_state = jnp.exp(b_ref[TOK - 1 :, hk]) * state + end_ref[:V, :K]
    later = jnp.sum(end_state * grad, axis=0, keepdims=True)
    terms = q_ref[:, hk].astype(F32) * dq - k_ref[:, hk].astype(F32) * dk
    r = lax.broadcasted_iota(jnp.int32, (TOK, TOK), 0)
    c = lax.broadcasted_iota(jnp.int32, (TOK, TOK), 1)
    ones = jnp.where(c >= r, 1.0, 0.0).astype(BF16)
    dg_ref[...] = folded(nn(ones, pair(terms))) + later
    stored(3)


def own_grads_kernel(q_ref, k_ref, v_ref, do_ref, b_ref, own_ref, in_ref, *rest):
    core = core_index()
    args = (q_ref, k_ref, v_ref, do_ref, b_ref)
    head_grads(core, *args, own_ref, in_ref, *rest[:6], *rest[6:10], lambda n: None)
    outer_gates(k_ref, b_ref, 1 - core, *rest[13:])
    inner_pairs(*args, 1 - core, *rest[10:13])


def final_kernel(q_ref, k_ref, v_ref, do_ref, b_ref, sent_ref, in_ref, *rest):
    inner_refs, mine, outs, theirs, sems = rest[:6], rest[6:10], rest[10:14], rest[14:18], rest[18]
    core = core_index()
    widths = (K, K, V, K)

    def copies(sources, h, base):
        return [
            pltpu.make_async_copy(source, out.at[:, at_head(h, width)], sems.at[base + n])
            for n, (source, out, width) in enumerate(zip(sources, outs, widths))
        ]

    first = copies(mine, core, 0)
    second = copies(theirs, 1 - core, 4)
    for copy in first:
        copy.start()
    head_grads(
        1 - core, q_ref, k_ref, v_ref, do_ref, b_ref, sent_ref, in_ref, *inner_refs, *theirs,
        lambda n: second[n].start(),
    )
    for copy in first + second:
        copy.wait()


VMEM = pl.BlockSpec(memory_space=pltpu.VMEM)
HBM = pl.BlockSpec(memory_space=pltpu.HBM)
SQUARE = ((TOK, HK), F32)
SQUARE16 = ((TOK, HK), BF16)
WIDE16 = ((TOK, HV), BF16)
HALF = ((TOK, K), F32)
INNER = [HALF, HALF, ((TOK, V), F32), HALF, HALF, ((TOK, 2 * K), BF16)]
HALF_GRADS = [((TOK, K), BF16), ((TOK, K), BF16), ((TOK, V), BF16), HALF]


def call(kernel, outs, *args, specs=None, out_specs=None, scratch=(), flops=1000000):
    shapes = [jax.ShapeDtypeStruct(shape, dtype) for shape, dtype in outs]
    out = pl.pallas_call(
        kernel,
        out_shape=shapes,
        in_specs=specs or [VMEM] * len(args),
        out_specs=out_specs or [VMEM] * len(outs),
        scratch_shapes=list(scratch),
        cost_estimate=pl.CostEstimate(flops=flops, bytes_accessed=2000000, transcendentals=0),
        compiler_params=pltpu.CompilerParams(vmem_limit_bytes=32 << 20),
    )(*args)
    return out if len(outs) > 1 else out[0]


def local(q, k, v, log_decay, do):
    q, k, v, do, log_decay = (
        pltpu.with_memory_space_constraint(x, pltpu.HBM) for x in (q, k, v, do, log_decay)
    )
    q, k, v, do, b, send = call(
        first_kernel,
        [SQUARE16, SQUARE16, WIDE16, WIDE16, SQUARE, ((V + 8, HK), F32)],
        q, k, v, do, log_decay,
        specs=[HBM] * 5,
        scratch=[pltpu.VMEM((TOK, HK), F32), pltpu.SemaphoreType.DMA((5,))],
    )
    got = lax.ppermute(send, "seq", SWAP)
    own, *inner = call(second_kernel, [SQUARE, *INNER], q, k, v, do, b, flops=100000000)
    msg = call(message_kernel, [((CHIPS * MSG, 1, HK), F32)], own, got, b)
    msg = exchanged(msg)
    back = call(scan_kernel, [SQUARE], msg)
    came = exchanged(back.reshape(CHIPS, ROWS, HK)).reshape(V, HK)
    onward, mine = call(onward_kernel, [SQUARE, SQUARE], own, got, b, came)
    theirs = lax.ppermute(onward, "seq", SWAP)
    done = call(
        own_grads_kernel,
        HALF_GRADS + INNER,
        q, k, v, do, b, own, mine, *inner,
        flops=100000000,
    )
    return call(
        final_kernel,
        [SQUARE16, SQUARE16, WIDE16, SQUARE],
        q, k, v, do, b, send, theirs, *done[4:], *done[:4],
        out_specs=[HBM] * 4,
        scratch=[pltpu.VMEM(*out) for out in HALF_GRADS] + [pltpu.SemaphoreType.DMA((8,))],
    )


def solution(mesh):
    return jax.shard_map(
        local, mesh=mesh, in_specs=(SPEC,) * 5, out_specs=(SPEC,) * 4, check_vma=False
    )
```

```python
import jax
import jax.numpy as jnp
from jax import lax
from jax.experimental import pallas as pl
from jax.experimental.pallas import tpu as pltpu
from jax.sharding import PartitionSpec as P

H = 2
K = 128
V = 256
GROUP = 64
TOK = 256
HK = H * K
HV = H * V
Y, Z, CORES = 4, 8, 2
CHIPS = Y * Z
ROWS = V // CHIPS
MSG = 2 * ROWS + 1
SPEC = P(("batch", "seq"), None)
FIRST = (Y // 2, Z // 2)


def steps(chip):
    y, z = (chip // Z - FIRST[0]) % Y, (chip % Z - FIRST[1]) % Z
    return min(y, Y - y) + min(z, Z - z)


LISTED = sorted(range(CHIPS), key=steps)
GROUPS = [[CORES * chip + core for chip in LISTED] for core in range(CORES)]
LAG_NS = 900
SWAP = [(device, device ^ 1) for device in range(CHIPS * CORES)]
F32 = jnp.float32
BF16 = jnp.bfloat16


def core_index():
    return lax.rem(lax.axis_index("seq"), CORES)


def exchanged(x):
    return lax.all_to_all(x, "seq", 0, 0, axis_index_groups=GROUPS, tiled=True)


def dot(left, right, dims):
    return lax.dot_general(left, right, (dims, ((), ())), preferred_element_type=F32)


def nn(left, right):
    return dot(left, right, ((1,), (0,)))


def nt(left, right):
    return dot(left, right, ((1,), (1,)))


def tn(left, right):
    return dot(left, right, ((0,), (0,)))


def split(x):
    hi = x.astype(BF16)
    return hi, (x - hi.astype(F32)).astype(BF16)


def pair(x):
    return jnp.concatenate(split(x), 1)


def folded(out):
    half = out.shape[1] // 2
    return out[:, :half] + out[:, half:]


def running_sum(x):
    rows = x.shape[0]
    r = lax.broadcasted_iota(jnp.int32, (rows, rows), 0)
    c = lax.broadcasted_iota(jnp.int32, (rows, rows), 1)
    ones = jnp.where(c <= r, 1.0, 0.0).astype(BF16)
    hi = x.astype(BF16)
    mid, lo = split(x - hi.astype(F32))
    return folded(nn(ones, halves(hi, mid))) + nn(ones, lo)


def head(h, width):
    return slice(h * width, (h + 1) * width)


def at_head(h, width):
    return pl.ds(pl.multiple_of(h * width, width), width)


def halves(left, right):
    return jnp.concatenate((left, right), 1)


def block_ends(q_ref, k_ref, v_ref, do_ref, b_ref, out_ref, h):
    hk, hv = at_head(h, K), at_head(h, V)
    b = b_ref[...]
    total = b_ref[TOK - 1 :]
    out_ref[:V, :K] = folded(tn(v_ref[:, hv], pair(k_ref[:, hk].astype(F32) * jnp.exp(total - b))))
    out_ref[:V, K:] = folded(tn(do_ref[:, hv], pair(q_ref[:, hk].astype(F32) * jnp.exp(b))))


def first_kernel(
    q_hbm, k_hbm, v_hbm, do_hbm, g_hbm, q_ref, k_ref, v_ref, do_ref, g_ref, b_ref, send_ref, sems
):
    core = core_index()
    pieces = ((g_hbm, g_ref, K), (k_hbm, k_ref, K), (v_hbm, v_ref, V), (q_hbm, q_ref, K), (do_hbm, do_ref, V))

    def copies(h, base):
        return [
            pltpu.make_async_copy(
                source.at[:, at_head(h, width)], target.at[:, at_head(h, width)], sems.at[base + n]
            )
            for n, (source, target, width) in enumerate(pieces)
        ]

    sent, kept = copies(1 - core, 0), copies(core, len(pieces))
    for copy in sent + kept:
        copy.start()
    sent[0].wait()
    b_ref[...] = running_sum(g_ref[:, at_head(1 - core, K)])
    for copy in sent[1:]:
        copy.wait()
    block_ends(q_ref, k_ref, v_ref, do_ref, b_ref, send_ref, 1 - core)
    total = b_ref[TOK - 1 :]
    send_ref[V:] = jnp.broadcast_to(halves(total, total), (8, HK))
    for copy in kept:
        copy.wait()


def inner_pairs(q_ref, k_ref, v_ref, do_ref, b_ref, h, dq_ref, dk_ref, dv_ref):
    hk, hv = at_head(h, K), at_head(h, V)
    r = lax.broadcasted_iota(jnp.int32, (TOK, TOK), 0)
    c = lax.broadcasted_iota(jnp.int32, (TOK, TOK), 1)
    q = q_ref[:, hk].astype(F32)
    k = k_ref[:, hk].astype(F32)
    b = b_ref[...]
    v = v_ref[:, hv]
    do = do_ref[:, hv]
    p_hi, p_lo = split(jnp.where(c <= r, nt(do, v), 0.0))
    t_hi, t_lo = split(jnp.where(c >= r, nt(v, do), 0.0))
    dk = jnp.zeros((TOK, K), F32)
    dv = jnp.zeros((TOK, V), F32)
    for i in range(TOK // GROUP):
        rows = slice(i * GROUP, (i + 1) * GROUP)
        end = (i + 1) * GROUP
        upto = slice(0, end)
        start = b[i * GROUP - 1 : i * GROUP] if i else jnp.zeros((1, K), F32)
        rising = jnp.exp(b[rows] - start)
        falling = jnp.exp(start - b[upto])
        q_hi, q_lo = split(q[rows] * rising)
        k_hi, k_lo = split(k[upto] * falling)
        scores_t = nt(k_hi, q_hi) + (nt(k_hi, q_lo) + nt(k_lo, q_hi))
        rr = lax.broadcasted_iota(jnp.int32, (end, GROUP), 0)
        cc = lax.broadcasted_iota(jnp.int32, (end, GROUP), 1) + i * GROUP
        s_hi, s_lo = split(jnp.where(cc >= rr, scores_t, 0.0))
        dq_ref[rows] = rising * (
            folded(nn(p_hi[rows, upto], halves(k_hi, k_lo))) + nn(p_lo[rows, upto], k_hi)
        )
        dk_part = falling * (
            folded(nn(t_hi[upto, rows], halves(q_hi, q_lo))) + nn(t_lo[upto, rows], q_hi)
        )
        dv_part = nn(s_hi, do[rows]) + nn(s_lo, do[rows])
        if end < TOK:
            dk_part = jnp.concatenate((dk_part, jnp.zeros((TOK - end, K), F32)), 0)
            dv_part = jnp.concatenate((dv_part, jnp.zeros((TOK - end, V), F32)), 0)
        dk = dk + dk_part
        dv = dv + dv_part
    dk_ref[...] = dk
    dv_ref[...] = dv


def outer_gates(k_ref, b_ref, h, rise_ref, tail_ref, kt_ref):
    b = b_ref[...]
    tail = jnp.exp(b_ref[TOK - 1 :] - b)
    rise_ref[...] = jnp.exp(b)
    tail_ref[...] = tail
    kt_ref[...] = pair(k_ref[:, at_head(h, K)].astype(F32) * tail)


def second_kernel(q_ref, k_ref, v_ref, do_ref, g_ref, b_ref, own_ref, *inner_refs):
    core = core_index()
    b_ref[...] = running_sum(g_ref[:, at_head(core, K)])
    block_ends(q_ref, k_ref, v_ref, do_ref, b_ref, own_ref, core)
    outer_gates(k_ref, b_ref, core, *inner_refs[3:])
    inner_pairs(q_ref, k_ref, v_ref, do_ref, b_ref, core, *inner_refs[:3])


def lane_gates(b_ref, got_ref):
    core = core_index()
    total = b_ref[TOK - 1 :]
    mine = jnp.exp(halves(total, total))
    other = jnp.exp(got_ref[V : V + 1])
    forward = lax.broadcasted_iota(jnp.int32, (1, HK), 1) < K
    return mine, other, forward, core == 0


def pick(flag, forward, when_true, when_false):
    return jnp.where(jnp.logical_xor(forward, jnp.logical_not(flag)), when_true, when_false)


def message_kernel(own_ref, got_ref, b_ref, msg_ref):
    @pl.when(core_index() == 0)
    def _():
        pl.delay(LAG_NS)

    mine, other, forward, first = lane_gates(b_ref, got_ref)
    own_gate = pick(first, forward, other, 1.0)
    got_gate = pick(first, forward, 1.0, mine)
    for i in range(CHIPS):
        rows = slice(i * ROWS, (i + 1) * ROWS)
        chip = own_ref[rows] * own_gate + got_ref[rows] * got_gate
        for side in range(2):
            at = i * MSG + side * ROWS
            msg_ref[at : at + ROWS, 0, :] = chip[:, head(side, K)]
        msg_ref[i * MSG + 2 * ROWS] = (mine * other)[:, :K]


def scan_kernel(msg_ref, out_ref):
    places = [LISTED.index(chip) for chip in range(CHIPS)]
    for side, order in enumerate((places, places[::-1])):
        state = jnp.zeros((ROWS, K), F32)
        for i in order:
            out_ref[i * ROWS : (i + 1) * ROWS, head(side, K)] = state
            at = i * MSG + side * ROWS
            state = msg_ref[i * MSG + 2 * ROWS] * state + msg_ref[at : at + ROWS, 0, :]


def onward_kernel(own_ref, got_ref, b_ref, came_ref, send_ref, mine_ref):
    mine, other, forward, first = lane_gates(b_ref, got_ref)
    came = came_ref[...]
    send_ref[...] = came * pick(first, forward, mine, 1.0) + pick(
        first, forward, own_ref[...], 0.0
    )
    mine_ref[...] = came * pick(first, forward, 1.0, other) + pick(
        first, forward, 0.0, got_ref[:V]
    )


def head_grads(
    h, q_ref, k_ref, v_ref, do_ref, b_ref, end_ref, in_ref,
    dqi_ref, dki_ref, dvi_ref, rise_ref, tail_ref, kt_ref, dq_ref, dk_ref, dv_ref, dg_ref, stored,
):
    hk, hv = at_head(h, K), at_head(h, V)
    state = in_ref[:, :K]
    grad = in_ref[:, K:]
    g_hi, g_lo = split(grad)
    dq = dqi_ref[...] + rise_ref[...] * folded(nn(do_ref[:, hv], pair(state)))
    dk = dki_ref[...] + tail_ref[...] * folded(nn(v_ref[:, hv], halves(g_hi, g_lo)))
    dq_ref[...] = dq.astype(BF16)
    stored(0)
    dk_ref[...] = dk.astype(BF16)
    stored(1)
    dv = dvi_ref[...] + (nt(kt_ref[...], halves(g_hi, g_hi)) + nt(kt_ref[:, :K], g_lo))
    dv_ref[...] = dv.astype(BF16)
    stored(2)
    end_state = jnp.exp(b_ref[TOK - 1 :]) * state + end_ref[:V, :K]
    later = jnp.sum(end_state * grad, axis=0, keepdims=True)
    terms = q_ref[:, hk].astype(F32) * dq - k_ref[:, hk].astype(F32) * dk
    r = lax.broadcasted_iota(jnp.int32, (TOK, TOK), 0)
    c = lax.broadcasted_iota(jnp.int32, (TOK, TOK), 1)
    ones = jnp.where(c >= r, 1.0, 0.0).astype(BF16)
    dg_ref[...] = folded(nn(ones, pair(terms))) + later
    stored(3)


def own_grads_kernel(q_ref, k_ref, v_ref, do_ref, b_ref, b_sent_ref, own_ref, in_ref, *rest):
    core = core_index()
    args = (q_ref, k_ref, v_ref, do_ref)
    head_grads(core, *args, b_ref, own_ref, in_ref, *rest[:6], *rest[6:10], lambda n: None)
    outer_gates(k_ref, b_sent_ref, 1 - core, *rest[13:])
    inner_pairs(*args, b_sent_ref, 1 - core, *rest[10:13])


def final_kernel(q_ref, k_ref, v_ref, do_ref, b_ref, sent_ref, in_ref, *rest):
    inner_refs, mine, outs, theirs, sems = rest[:6], rest[6:10], rest[10:14], rest[14:18], rest[18]
    core = core_index()
    widths = (K, K, V, K)

    def copies(sources, h, base):
        return [
            pltpu.make_async_copy(source, out.at[:, at_head(h, width)], sems.at[base + n])
            for n, (source, out, width) in enumerate(zip(sources, outs, widths))
        ]

    first = copies(mine, core, 0)
    second = copies(theirs, 1 - core, 4)
    for copy in first:
        copy.start()
    head_grads(
        1 - core, q_ref, k_ref, v_ref, do_ref, b_ref, sent_ref, in_ref, *inner_refs, *theirs,
        lambda n: second[n].start(),
    )
    for copy in first + second:
        copy.wait()


VMEM = pl.BlockSpec(memory_space=pltpu.VMEM)
HBM = pl.BlockSpec(memory_space=pltpu.HBM)
SQUARE = ((TOK, HK), F32)
SQUARE16 = ((TOK, HK), BF16)
WIDE16 = ((TOK, HV), BF16)
HALF = ((TOK, K), F32)
INNER = [HALF, HALF, ((TOK, V), F32), HALF, HALF, ((TOK, 2 * K), BF16)]
HALF_GRADS = [((TOK, K), BF16), ((TOK, K), BF16), ((TOK, V), BF16), HALF]


def call(kernel, outs, *args, specs=None, out_specs=None, scratch=(), flops=1000000):
    shapes = [jax.ShapeDtypeStruct(shape, dtype) for shape, dtype in outs]
    out = pl.pallas_call(
        kernel,
        out_shape=shapes,
        in_specs=specs or [VMEM] * len(args),
        out_specs=out_specs or [VMEM] * len(outs),
        scratch_shapes=list(scratch),
        cost_estimate=pl.CostEstimate(flops=flops, bytes_accessed=2000000, transcendentals=0),
        compiler_params=pltpu.CompilerParams(vmem_limit_bytes=32 << 20),
    )(*args)
    return out if len(outs) > 1 else out[0]


def local(q, k, v, log_decay, do):
    q, k, v, do, log_decay = (
        pltpu.with_memory_space_constraint(x, pltpu.HBM) for x in (q, k, v, do, log_decay)
    )
    q, k, v, do, log_decay, b_sent, send = call(
        first_kernel,
        [SQUARE16, SQUARE16, WIDE16, WIDE16, SQUARE, HALF, ((V + 8, HK), F32)],
        q, k, v, do, log_decay,
        specs=[HBM] * 5,
        scratch=[pltpu.SemaphoreType.DMA((10,))],
    )
    got = lax.ppermute(send, "seq", SWAP)
    b, own, *inner = call(
        second_kernel, [HALF, SQUARE, *INNER], q, k, v, do, log_decay, flops=100000000
    )
    msg = call(message_kernel, [((CHIPS * MSG, 1, K), F32)], own, got, b)
    msg = exchanged(msg)
    back = call(scan_kernel, [SQUARE], msg)
    came = exchanged(back.reshape(CHIPS, ROWS, HK)).reshape(V, HK)
    onward, mine = call(onward_kernel, [SQUARE, SQUARE], own, got, b, came)
    theirs = lax.ppermute(onward, "seq", SWAP)
    done = call(
        own_grads_kernel,
        HALF_GRADS + INNER,
        q, k, v, do, b, b_sent, own, mine, *inner,
        flops=100000000,
    )
    return call(
        final_kernel,
        [SQUARE16, SQUARE16, WIDE16, SQUARE],
        q, k, v, do, b_sent, send, theirs, *done[4:], *done[:4],
        out_specs=[HBM] * 4,
        scratch=[pltpu.VMEM(*out) for out in HALF_GRADS] + [pltpu.SemaphoreType.DMA((8,))],
    )


def solution(mesh):
    return jax.shard_map(
        local, mesh=mesh, in_specs=(SPEC,) * 5, out_specs=(SPEC,) * 4, check_vma=False
    )
```

```python
import jax
import jax.numpy as jnp
from jax import lax
from jax.experimental import pallas as pl
from jax.experimental.pallas import tpu as pltpu
from jax.sharding import PartitionSpec as P

H = 2
K = 128
V = 256
GROUP = 64
TOK = 256
HK = H * K
HV = H * V
Y, Z, CORES = 4, 8, 2
CHIPS = Y * Z
ROWS = V // CHIPS
MSG = 2 * ROWS + 1
SPEC = P(("batch", "seq"), None)
FIRST = (Y // 2, Z // 2)


def steps(chip):
    y, z = (chip // Z - FIRST[0]) % Y, (chip % Z - FIRST[1]) % Z
    return min(y, Y - y) + min(z, Z - z)


LISTED = sorted(range(CHIPS), key=steps)
GROUPS = [[CORES * chip + core for chip in LISTED] for core in range(CORES)]
SWAP = [(device, device ^ 1) for device in range(CHIPS * CORES)]
F32 = jnp.float32
BF16 = jnp.bfloat16


def core_index():
    return lax.rem(lax.axis_index("seq"), CORES)


def exchanged(x):
    return lax.all_to_all(x, "seq", 0, 0, axis_index_groups=GROUPS, tiled=True)


def dot(left, right, dims):
    return lax.dot_general(left, right, (dims, ((), ())), preferred_element_type=F32)


def nn(left, right):
    return dot(left, right, ((1,), (0,)))


def nt(left, right):
    return dot(left, right, ((1,), (1,)))


def tn(left, right):
    return dot(left, right, ((0,), (0,)))


def split(x):
    hi = x.astype(BF16)
    return hi, (x - hi.astype(F32)).astype(BF16)


def pair(x):
    return jnp.concatenate(split(x), 1)


def folded(out):
    half = out.shape[1] // 2
    return out[:, :half] + out[:, half:]


def running_sum(x):
    rows = x.shape[0]
    r = lax.broadcasted_iota(jnp.int32, (rows, rows), 0)
    c = lax.broadcasted_iota(jnp.int32, (rows, rows), 1)
    ones = jnp.where(c <= r, 1.0, 0.0).astype(BF16)
    hi = x.astype(BF16)
    mid, lo = split(x - hi.astype(F32))
    return folded(nn(ones, halves(hi, mid))) + nn(ones, lo)


def head(h, width):
    return slice(h * width, (h + 1) * width)


def at_head(h, width):
    return pl.ds(pl.multiple_of(h * width, width), width)


def halves(left, right):
    return jnp.concatenate((left, right), 1)


def block_ends(q_ref, k_ref, v_ref, do_ref, b_ref, out_ref, h):
    hk, hv = at_head(h, K), at_head(h, V)
    b = b_ref[...]
    total = b_ref[TOK - 1 :]
    out_ref[:V, :K] = folded(tn(v_ref[:, hv], pair(k_ref[:, hk].astype(F32) * jnp.exp(total - b))))
    out_ref[:V, K:] = folded(tn(do_ref[:, hv], pair(q_ref[:, hk].astype(F32) * jnp.exp(b))))


def first_kernel(
    q_hbm, k_hbm, v_hbm, do_hbm, g_hbm, q_ref, k_ref, v_ref, do_ref, g_ref, b_ref, send_ref, sems
):
    core = core_index()
    pieces = ((g_hbm, g_ref, K), (k_hbm, k_ref, K), (v_hbm, v_ref, V), (q_hbm, q_ref, K), (do_hbm, do_ref, V))

    def copies(h, base):
        return [
            pltpu.make_async_copy(
                source.at[:, at_head(h, width)], target.at[:, at_head(h, width)], sems.at[base + n]
            )
            for n, (source, target, width) in enumerate(pieces)
        ]

    sent, kept = copies(1 - core, 0), copies(core, len(pieces))
    for copy in sent + kept:
        copy.start()
    sent[0].wait()
    b_ref[...] = running_sum(g_ref[:, at_head(1 - core, K)])
    for copy in sent[1:]:
        copy.wait()
    block_ends(q_ref, k_ref, v_ref, do_ref, b_ref, send_ref, 1 - core)
    total = b_ref[TOK - 1 :]
    send_ref[V:] = jnp.broadcast_to(halves(total, total), (8, HK))
    for copy in kept:
        copy.wait()


def inner_pairs(q_ref, k_ref, v_ref, do_ref, b_ref, h, dq_ref, dk_ref, dv_ref):
    hk, hv = at_head(h, K), at_head(h, V)
    r = lax.broadcasted_iota(jnp.int32, (TOK, TOK), 0)
    c = lax.broadcasted_iota(jnp.int32, (TOK, TOK), 1)
    q = q_ref[:, hk].astype(F32)
    k = k_ref[:, hk].astype(F32)
    b = b_ref[...]
    v = v_ref[:, hv]
    do = do_ref[:, hv]
    p_hi, p_lo = split(jnp.where(c <= r, nt(do, v), 0.0))
    t_hi, t_lo = split(jnp.where(c >= r, nt(v, do), 0.0))
    dk = jnp.zeros((TOK, K), F32)
    dv = jnp.zeros((TOK, V), F32)
    for i in range(TOK // GROUP):
        rows = slice(i * GROUP, (i + 1) * GROUP)
        end = (i + 1) * GROUP
        upto = slice(0, end)
        start = b[i * GROUP - 1 : i * GROUP] if i else jnp.zeros((1, K), F32)
        rising = jnp.exp(b[rows] - start)
        falling = jnp.exp(start - b[upto])
        q_hi, q_lo = split(q[rows] * rising)
        k_hi, k_lo = split(k[upto] * falling)
        scores_t = nt(k_hi, q_hi) + (nt(k_hi, q_lo) + nt(k_lo, q_hi))
        rr = lax.broadcasted_iota(jnp.int32, (end, GROUP), 0)
        cc = lax.broadcasted_iota(jnp.int32, (end, GROUP), 1) + i * GROUP
        s_hi, s_lo = split(jnp.where(cc >= rr, scores_t, 0.0))
        dq_ref[rows] = rising * (
            folded(nn(p_hi[rows, upto], halves(k_hi, k_lo))) + nn(p_lo[rows, upto], k_hi)
        )
        dk_part = falling * (
            folded(nn(t_hi[upto, rows], halves(q_hi, q_lo))) + nn(t_lo[upto, rows], q_hi)
        )
        dv_part = nn(s_hi, do[rows]) + nn(s_lo, do[rows])
        if end < TOK:
            dk_part = jnp.concatenate((dk_part, jnp.zeros((TOK - end, K), F32)), 0)
            dv_part = jnp.concatenate((dv_part, jnp.zeros((TOK - end, V), F32)), 0)
        dk = dk + dk_part
        dv = dv + dv_part
    dk_ref[...] = dk
    dv_ref[...] = dv


def outer_gates(k_ref, b_ref, h, rise_ref, tail_ref, kt_ref):
    b = b_ref[...]
    tail = jnp.exp(b_ref[TOK - 1 :] - b)
    rise_ref[...] = jnp.exp(b)
    tail_ref[...] = tail
    kt_ref[...] = pair(k_ref[:, at_head(h, K)].astype(F32) * tail)


def both_inner(q_ref, k_ref, v_ref, do_ref, b_ref, b_sent_ref, core, inner_refs):
    for h, sums_ref, refs in ((core, b_ref, inner_refs[:6]), (1 - core, b_sent_ref, inner_refs[6:])):
        inner_pairs(q_ref, k_ref, v_ref, do_ref, sums_ref, h, *refs[:3])
        outer_gates(k_ref, sums_ref, h, *refs[3:])


def second_kernel(q_ref, k_ref, v_ref, do_ref, g_ref, b_sent_ref, b_ref, own_ref, *inner_refs):
    core = core_index()
    b_ref[...] = running_sum(g_ref[:, at_head(core, K)])
    block_ends(q_ref, k_ref, v_ref, do_ref, b_ref, own_ref, core)

    @pl.when(core == 0)
    def _():
        both_inner(q_ref, k_ref, v_ref, do_ref, b_ref, b_sent_ref, core, inner_refs)


def lane_gates(b_ref, got_ref):
    core = core_index()
    total = b_ref[TOK - 1 :]
    mine = jnp.exp(halves(total, total))
    other = jnp.exp(got_ref[V : V + 1])
    forward = lax.broadcasted_iota(jnp.int32, (1, HK), 1) < K
    return mine, other, forward, core == 0


def pick(flag, forward, when_true, when_false):
    return jnp.where(jnp.logical_xor(forward, jnp.logical_not(flag)), when_true, when_false)


def message_kernel(own_ref, got_ref, b_ref, msg_ref):
    mine, other, forward, first = lane_gates(b_ref, got_ref)
    own_gate = pick(first, forward, other, 1.0)
    got_gate = pick(first, forward, 1.0, mine)
    for i in range(CHIPS):
        rows = slice(i * ROWS, (i + 1) * ROWS)
        chip = own_ref[rows] * own_gate + got_ref[rows] * got_gate
        for side in range(2):
            at = i * MSG + side * ROWS
            msg_ref[at : at + ROWS, 0, :] = chip[:, head(side, K)]
        msg_ref[i * MSG + 2 * ROWS] = (mine * other)[:, :K]


def scan_kernel(msg_ref, out_ref):
    places = [LISTED.index(chip) for chip in range(CHIPS)]
    for side, order in enumerate((places, places[::-1])):
        state = jnp.zeros((ROWS, K), F32)
        for i in order:
            out_ref[i * ROWS : (i + 1) * ROWS, head(side, K)] = state
            at = i * MSG + side * ROWS
            state = msg_ref[i * MSG + 2 * ROWS] * state + msg_ref[at : at + ROWS, 0, :]


def onward_kernel(
    own_ref, got_ref, b_ref, came_ref, q_ref, k_ref, v_ref, do_ref, b_sent_ref, *rest
):
    send_ref, mine_ref = rest[12:14]
    core = core_index()
    mine, other, forward, first = lane_gates(b_ref, got_ref)
    came = came_ref[...]
    send_ref[...] = came * pick(first, forward, mine, 1.0) + pick(
        first, forward, own_ref[...], 0.0
    )
    mine_ref[...] = came * pick(first, forward, 1.0, other) + pick(
        first, forward, 0.0, got_ref[:V]
    )

    @pl.when(core == 1)
    def _():
        both_inner(q_ref, k_ref, v_ref, do_ref, b_ref, b_sent_ref, core, rest[14:])


def head_grads(
    h, q_ref, k_ref, v_ref, do_ref, b_ref, end_ref, in_ref,
    dqi_ref, dki_ref, dvi_ref, rise_ref, tail_ref, kt_ref, dq_ref, dk_ref, dv_ref, dg_ref, stored,
):
    hk, hv = at_head(h, K), at_head(h, V)
    state = in_ref[:, :K]
    grad = in_ref[:, K:]
    g_hi, g_lo = split(grad)
    dq = dqi_ref[...] + rise_ref[...] * folded(nn(do_ref[:, hv], pair(state)))
    dk = dki_ref[...] + tail_ref[...] * folded(nn(v_ref[:, hv], halves(g_hi, g_lo)))
    dq_ref[...] = dq.astype(BF16)
    stored(0)
    dk_ref[...] = dk.astype(BF16)
    stored(1)
    dv = dvi_ref[...] + (nt(kt_ref[...], halves(g_hi, g_hi)) + nt(kt_ref[:, :K], g_lo))
    dv_ref[...] = dv.astype(BF16)
    stored(2)
    end_state = jnp.exp(b_ref[TOK - 1 :]) * state + end_ref[:V, :K]
    later = jnp.sum(end_state * grad, axis=0, keepdims=True)
    terms = q_ref[:, hk].astype(F32) * dq - k_ref[:, hk].astype(F32) * dk
    r = lax.broadcasted_iota(jnp.int32, (TOK, TOK), 0)
    c = lax.broadcasted_iota(jnp.int32, (TOK, TOK), 1)
    ones = jnp.where(c >= r, 1.0, 0.0).astype(BF16)
    dg_ref[...] = folded(nn(ones, pair(terms))) + later
    stored(3)


def own_grads_kernel(q_ref, k_ref, v_ref, do_ref, b_ref, own_ref, in_ref, *rest):
    head_grads(
        core_index(), q_ref, k_ref, v_ref, do_ref, b_ref, own_ref, in_ref, *rest, lambda n: None
    )


def final_kernel(q_ref, k_ref, v_ref, do_ref, b_ref, sent_ref, in_ref, *rest):
    inner_refs, mine, outs, theirs, sems = rest[:6], rest[6:10], rest[10:14], rest[14:18], rest[18]
    core = core_index()
    widths = (K, K, V, K)

    def copies(sources, h, base):
        return [
            pltpu.make_async_copy(source, out.at[:, at_head(h, width)], sems.at[base + n])
            for n, (source, out, width) in enumerate(zip(sources, outs, widths))
        ]

    first = copies(mine, core, 0)
    second = copies(theirs, 1 - core, 4)
    for copy in first:
        copy.start()
    head_grads(
        1 - core, q_ref, k_ref, v_ref, do_ref, b_ref, sent_ref, in_ref, *inner_refs, *theirs,
        lambda n: second[n].start(),
    )
    for copy in first + second:
        copy.wait()


VMEM = pl.BlockSpec(memory_space=pltpu.VMEM)
HBM = pl.BlockSpec(memory_space=pltpu.HBM)
SQUARE = ((TOK, HK), F32)
SQUARE16 = ((TOK, HK), BF16)
WIDE16 = ((TOK, HV), BF16)
HALF = ((TOK, K), F32)
INNER = [HALF, HALF, ((TOK, V), F32), HALF, HALF, ((TOK, 2 * K), BF16)]
HALF_GRADS = [((TOK, K), BF16), ((TOK, K), BF16), ((TOK, V), BF16), HALF]


def call(kernel, outs, *args, specs=None, out_specs=None, scratch=(), flops=1000000, alias=None):
    shapes = [jax.ShapeDtypeStruct(shape, dtype) for shape, dtype in outs]
    out = pl.pallas_call(
        kernel,
        out_shape=shapes,
        in_specs=specs or [VMEM] * len(args),
        out_specs=out_specs or [VMEM] * len(outs),
        scratch_shapes=list(scratch),
        input_output_aliases=alias or {},
        cost_estimate=pl.CostEstimate(flops=flops, bytes_accessed=2000000, transcendentals=0),
        compiler_params=pltpu.CompilerParams(vmem_limit_bytes=32 << 20),
    )(*args)
    return out if len(outs) > 1 else out[0]


def local(q, k, v, log_decay, do):
    q, k, v, do, log_decay = (
        pltpu.with_memory_space_constraint(x, pltpu.HBM) for x in (q, k, v, do, log_decay)
    )
    q, k, v, do, log_decay, b_sent, send = call(
        first_kernel,
        [SQUARE16, SQUARE16, WIDE16, WIDE16, SQUARE, HALF, ((V + 8, HK), F32)],
        q, k, v, do, log_decay,
        specs=[HBM] * 5,
        scratch=[pltpu.SemaphoreType.DMA((10,))],
    )
    got = lax.ppermute(send, "seq", SWAP)
    b, own, *inner = call(
        second_kernel, [HALF, SQUARE, *INNER, *INNER], q, k, v, do, log_decay, b_sent,
        flops=100000000,
    )
    msg = call(message_kernel, [((CHIPS * MSG, 1, K), F32)], own, got, b)
    msg = exchanged(msg)
    back = call(scan_kernel, [SQUARE], msg)
    came = exchanged(back.reshape(CHIPS, ROWS, HK)).reshape(V, HK)
    onward, mine, *inner = call(
        onward_kernel,
        [SQUARE, SQUARE, *INNER, *INNER],
        own, got, b, came, q, k, v, do, b_sent, *inner,
        alias={9 + n: 2 + n for n in range(12)},
    )
    theirs = lax.ppermute(onward, "seq", SWAP)
    done = call(
        own_grads_kernel, HALF_GRADS, q, k, v, do, b, own, mine, *inner[:6], flops=100000000
    )
    return call(
        final_kernel,
        [SQUARE16, SQUARE16, WIDE16, SQUARE],
        q, k, v, do, b_sent, send, theirs, *inner[6:], *done,
        out_specs=[HBM] * 4,
        scratch=[pltpu.VMEM(*out) for out in HALF_GRADS] + [pltpu.SemaphoreType.DMA((8,))],
    )


def solution(mesh):
    return jax.shard_map(
        local, mesh=mesh, in_specs=(SPEC,) * 5, out_specs=(SPEC,) * 4, check_vma=False
    )
```

```python
import jax
import jax.numpy as jnp
from jax import lax
from jax.experimental import pallas as pl
from jax.experimental.pallas import tpu as pltpu
from jax.sharding import PartitionSpec as P

H = 2
K = 128
V = 256
GROUP = 64
TOK = 256
HK = H * K
HV = H * V
Y, Z, CORES = 4, 8, 2
CHIPS = Y * Z
ROWS = V // CHIPS
MSG = 2 * ROWS + 1
SPEC = P(("batch", "seq"), None)
FIRST = (Y // 2, Z // 2)


def steps(chip):
    y, z = (chip // Z - FIRST[0]) % Y, (chip % Z - FIRST[1]) % Z
    return min(y, Y - y) + min(z, Z - z)


LISTED = sorted(range(CHIPS), key=steps)
GROUPS = [[CORES * chip + core for chip in LISTED] for core in range(CORES)]
SWAP = [(device, device ^ 1) for device in range(CHIPS * CORES)]
F32 = jnp.float32
BF16 = jnp.bfloat16


def core_index():
    return lax.rem(lax.axis_index("seq"), CORES)


def exchanged(x):
    return lax.all_to_all(x, "seq", 0, 0, axis_index_groups=GROUPS, tiled=True)


def dot(left, right, dims):
    return lax.dot_general(left, right, (dims, ((), ())), preferred_element_type=F32)


def nn(left, right):
    return dot(left, right, ((1,), (0,)))


def nt(left, right):
    return dot(left, right, ((1,), (1,)))


def tn(left, right):
    return dot(left, right, ((0,), (0,)))


def split(x):
    hi = x.astype(BF16)
    return hi, (x - hi.astype(F32)).astype(BF16)


def pair(x):
    return jnp.concatenate(split(x), 1)


def folded(out):
    half = out.shape[1] // 2
    return out[:, :half] + out[:, half:]


def running_sum(x):
    rows = x.shape[0]
    r = lax.broadcasted_iota(jnp.int32, (rows, rows), 0)
    c = lax.broadcasted_iota(jnp.int32, (rows, rows), 1)
    ones = jnp.where(c <= r, 1.0, 0.0).astype(BF16)
    hi = x.astype(BF16)
    mid, lo = split(x - hi.astype(F32))
    return folded(nn(ones, halves(hi, mid))) + nn(ones, lo)


def head(h, width):
    return slice(h * width, (h + 1) * width)


def at_head(h, width):
    return pl.ds(pl.multiple_of(h * width, width), width)


def halves(left, right):
    return jnp.concatenate((left, right), 1)


def block_ends(q_ref, k_ref, v_ref, do_ref, b_ref, out_ref, h):
    hk, hv = at_head(h, K), at_head(h, V)
    b = b_ref[...]
    total = b_ref[TOK - 1 :]
    out_ref[:V, :K] = folded(tn(v_ref[:, hv], pair(k_ref[:, hk].astype(F32) * jnp.exp(total - b))))
    out_ref[:V, K:] = folded(tn(do_ref[:, hv], pair(q_ref[:, hk].astype(F32) * jnp.exp(b))))


def first_kernel(
    q_hbm, k_hbm, v_hbm, do_hbm, g_hbm, q_ref, k_ref, v_ref, do_ref, g_ref, b_ref, send_ref, sems
):
    core = core_index()
    pieces = ((g_hbm, g_ref, K), (k_hbm, k_ref, K), (v_hbm, v_ref, V), (q_hbm, q_ref, K), (do_hbm, do_ref, V))

    def copies(h, base):
        return [
            pltpu.make_async_copy(
                source.at[:, at_head(h, width)], target.at[:, at_head(h, width)], sems.at[base + n]
            )
            for n, (source, target, width) in enumerate(pieces)
        ]

    sent, kept = copies(1 - core, 0), copies(core, len(pieces))
    for copy in sent + kept:
        copy.start()
    sent[0].wait()
    b_ref[...] = running_sum(g_ref[:, at_head(1 - core, K)])
    for copy in sent[1:]:
        copy.wait()
    block_ends(q_ref, k_ref, v_ref, do_ref, b_ref, send_ref, 1 - core)
    total = b_ref[TOK - 1 :]
    send_ref[V:] = jnp.broadcast_to(halves(total, total), (8, HK))
    for copy in kept:
        copy.wait()


def inner_pairs(q_ref, k_ref, v_ref, do_ref, b_ref, h, dq_ref, dk_ref, dv_ref):
    hk, hv = at_head(h, K), at_head(h, V)
    r = lax.broadcasted_iota(jnp.int32, (TOK, TOK), 0)
    c = lax.broadcasted_iota(jnp.int32, (TOK, TOK), 1)
    q = q_ref[:, hk].astype(F32)
    k = k_ref[:, hk].astype(F32)
    b = b_ref[...]
    v = v_ref[:, hv]
    do = do_ref[:, hv]
    p_hi, p_lo = split(jnp.where(c <= r, nt(do, v), 0.0))
    t_hi, t_lo = split(jnp.where(c >= r, nt(v, do), 0.0))
    dk = jnp.zeros((TOK, K), F32)
    dv = jnp.zeros((TOK, V), F32)
    for i in range(TOK // GROUP):
        rows = slice(i * GROUP, (i + 1) * GROUP)
        end = (i + 1) * GROUP
        upto = slice(0, end)
        start = b[i * GROUP - 1 : i * GROUP] if i else jnp.zeros((1, K), F32)
        rising = jnp.exp(b[rows] - start)
        falling = jnp.exp(start - b[upto])
        q_hi, q_lo = split(q[rows] * rising)
        k_hi, k_lo = split(k[upto] * falling)
        scores_t = nt(k_hi, q_hi) + (nt(k_hi, q_lo) + nt(k_lo, q_hi))
        rr = lax.broadcasted_iota(jnp.int32, (end, GROUP), 0)
        cc = lax.broadcasted_iota(jnp.int32, (end, GROUP), 1) + i * GROUP
        s_hi, s_lo = split(jnp.where(cc >= rr, scores_t, 0.0))
        dq_ref[rows] = rising * (
            folded(nn(p_hi[rows, upto], halves(k_hi, k_lo))) + nn(p_lo[rows, upto], k_hi)
        )
        dk_part = falling * (
            folded(nn(t_hi[upto, rows], halves(q_hi, q_lo))) + nn(t_lo[upto, rows], q_hi)
        )
        dv_part = nn(s_hi, do[rows]) + nn(s_lo, do[rows])
        if end < TOK:
            dk_part = jnp.concatenate((dk_part, jnp.zeros((TOK - end, K), F32)), 0)
            dv_part = jnp.concatenate((dv_part, jnp.zeros((TOK - end, V), F32)), 0)
        dk = dk + dk_part
        dv = dv + dv_part
    dk_ref[...] = dk
    dv_ref[...] = dv


def outer_gates(k_ref, b_ref, h, rise_ref, tail_ref, kt_ref):
    b = b_ref[...]
    tail = jnp.exp(b_ref[TOK - 1 :] - b)
    rise_ref[...] = jnp.exp(b)
    tail_ref[...] = tail
    kt_ref[...] = pair(k_ref[:, at_head(h, K)].astype(F32) * tail)


def both_inner(q_ref, k_ref, v_ref, do_ref, b_ref, b_sent_ref, core, inner_refs):
    for h, sums_ref, refs in ((core, b_ref, inner_refs[:6]), (1 - core, b_sent_ref, inner_refs[6:])):
        inner_pairs(q_ref, k_ref, v_ref, do_ref, sums_ref, h, *refs[:3])
        outer_gates(k_ref, sums_ref, h, *refs[3:])


def second_kernel(q_ref, k_ref, v_ref, do_ref, g_ref, b_sent_ref, b_ref, own_ref, *inner_refs):
    core = core_index()
    b_ref[...] = running_sum(g_ref[:, at_head(core, K)])
    block_ends(q_ref, k_ref, v_ref, do_ref, b_ref, own_ref, core)

    @pl.when(core == 0)
    def _():
        both_inner(q_ref, k_ref, v_ref, do_ref, b_ref, b_sent_ref, core, inner_refs)


def lane_gates(b_ref, got_ref):
    core = core_index()
    total = b_ref[TOK - 1 :]
    mine = jnp.exp(halves(total, total))
    other = jnp.exp(got_ref[V : V + 1])
    forward = lax.broadcasted_iota(jnp.int32, (1, HK), 1) < K
    return mine, other, forward, core == 0


def pick(flag, forward, when_true, when_false):
    return jnp.where(jnp.logical_xor(forward, jnp.logical_not(flag)), when_true, when_false)


def message_kernel(own_ref, got_ref, b_ref, msg_ref):
    mine, other, forward, first = lane_gates(b_ref, got_ref)
    own_gate = pick(first, forward, other, 1.0)
    got_gate = pick(first, forward, 1.0, mine)
    for i in range(CHIPS):
        rows = slice(i * ROWS, (i + 1) * ROWS)
        chip = own_ref[rows] * own_gate + got_ref[rows] * got_gate
        for side in range(2):
            at = i * MSG + side * ROWS
            msg_ref[at : at + ROWS, 0, :] = chip[:, head(side, K)]
        msg_ref[i * MSG + 2 * ROWS] = (mine * other)[:, :K]


def scan_kernel(msg_ref, out_ref):
    places = [LISTED.index(chip) for chip in range(CHIPS)]
    for side, order in enumerate((places, places[::-1])):
        state = jnp.zeros((ROWS, K), F32)
        for i in order:
            out_ref[i * ROWS : (i + 1) * ROWS, head(side, K)] = state
            at = i * MSG + side * ROWS
            state = msg_ref[i * MSG + 2 * ROWS] * state + msg_ref[at : at + ROWS, 0, :]


def onward_kernel(
    own_ref, got_ref, b_ref, came_ref, q_ref, k_ref, v_ref, do_ref, b_sent_ref, *rest
):
    send_ref, mine_ref = rest[12:14]
    core = core_index()
    mine, other, forward, first = lane_gates(b_ref, got_ref)
    came = came_ref[...]
    send_ref[...] = came * pick(first, forward, mine, 1.0) + pick(
        first, forward, own_ref[...], 0.0
    )
    mine_ref[...] = came * pick(first, forward, 1.0, other) + pick(
        first, forward, 0.0, got_ref[:V]
    )

    @pl.when(core == 1)
    def _():
        both_inner(q_ref, k_ref, v_ref, do_ref, b_ref, b_sent_ref, core, rest[14:])


def head_grads(
    h, q_ref, k_ref, v_ref, do_ref, b_ref, end_ref, in_ref,
    dqi_ref, dki_ref, dvi_ref, rise_ref, tail_ref, kt_ref, dq_ref, dk_ref, dv_ref, dg_ref, stored,
):
    hk, hv = at_head(h, K), at_head(h, V)
    state = in_ref[:, :K]
    grad = in_ref[:, K:]
    g_hi, g_lo = split(grad)
    dq = dqi_ref[...] + rise_ref[...] * folded(nn(do_ref[:, hv], pair(state)))
    dk = dki_ref[...] + tail_ref[...] * folded(nn(v_ref[:, hv], halves(g_hi, g_lo)))
    dq_ref[...] = dq.astype(BF16)
    stored(0)
    dk_ref[...] = dk.astype(BF16)
    stored(1)
    dv = dvi_ref[...] + (nt(kt_ref[...], halves(g_hi, g_hi)) + nt(kt_ref[:, :K], g_lo))
    dv_ref[...] = dv.astype(BF16)
    stored(2)
    end_state = jnp.exp(b_ref[TOK - 1 :]) * state + end_ref[:V, :K]
    later = jnp.sum(end_state * grad, axis=0, keepdims=True)
    terms = q_ref[:, hk].astype(F32) * dq - k_ref[:, hk].astype(F32) * dk
    r = lax.broadcasted_iota(jnp.int32, (TOK, TOK), 0)
    c = lax.broadcasted_iota(jnp.int32, (TOK, TOK), 1)
    ones = jnp.where(c >= r, 1.0, 0.0).astype(BF16)
    dg_ref[...] = folded(nn(ones, pair(terms))) + later
    stored(3)


def grads_kernel(own, q_ref, k_ref, v_ref, do_ref, b_ref, end_ref, in_ref, *rest):
    inner_refs, outs, halves_out, sems = rest[:6], rest[-9:-5], rest[-5:-1], rest[-1]
    core = core_index()
    h = core if own else 1 - core
    copies = [
        pltpu.make_async_copy(source, out.at[:, at_head(h, width)], sems.at[n])
        for n, (source, out, width) in enumerate(zip(halves_out, outs, (K, K, V, K)))
    ]
    head_grads(
        h, q_ref, k_ref, v_ref, do_ref, b_ref, end_ref, in_ref, *inner_refs, *halves_out,
        lambda n: copies[n].start(),
    )
    for copy in copies:
        copy.wait()


VMEM = pl.BlockSpec(memory_space=pltpu.VMEM)
HBM = pl.BlockSpec(memory_space=pltpu.HBM)
SQUARE = ((TOK, HK), F32)
SQUARE16 = ((TOK, HK), BF16)
WIDE16 = ((TOK, HV), BF16)
HALF = ((TOK, K), F32)
INNER = [HALF, HALF, ((TOK, V), F32), HALF, HALF, ((TOK, 2 * K), BF16)]
HALF_GRADS = [((TOK, K), BF16), ((TOK, K), BF16), ((TOK, V), BF16), HALF]


def call(kernel, outs, *args, specs=None, out_specs=None, scratch=(), flops=1000000, alias=None):
    shapes = [jax.ShapeDtypeStruct(shape, dtype) for shape, dtype in outs]
    out = pl.pallas_call(
        kernel,
        out_shape=shapes,
        in_specs=specs or [VMEM] * len(args),
        out_specs=out_specs or [VMEM] * len(outs),
        scratch_shapes=list(scratch),
        input_output_aliases=alias or {},
        cost_estimate=pl.CostEstimate(flops=flops, bytes_accessed=2000000, transcendentals=0),
        compiler_params=pltpu.CompilerParams(vmem_limit_bytes=32 << 20),
    )(*args)
    return out if len(outs) > 1 else out[0]


def grads(own, args, into=()):
    def kernel(*refs):
        grads_kernel(own, *refs)

    return call(
        kernel,
        [SQUARE16, SQUARE16, WIDE16, SQUARE],
        *args,
        *into,
        specs=[VMEM] * len(args) + [HBM] * len(into),
        out_specs=[HBM] * 4,
        scratch=[pltpu.VMEM(*out) for out in HALF_GRADS] + [pltpu.SemaphoreType.DMA((4,))],
        flops=100000000,
        alias={len(args) + n: n for n in range(len(into))},
    )


def local(q, k, v, log_decay, do):
    q, k, v, do, log_decay = (
        pltpu.with_memory_space_constraint(x, pltpu.HBM) for x in (q, k, v, do, log_decay)
    )
    q, k, v, do, log_decay, b_sent, send = call(
        first_kernel,
        [SQUARE16, SQUARE16, WIDE16, WIDE16, SQUARE, HALF, ((V + 8, HK), F32)],
        q, k, v, do, log_decay,
        specs=[HBM] * 5,
        scratch=[pltpu.SemaphoreType.DMA((10,))],
    )
    got = lax.ppermute(send, "seq", SWAP)
    b, own, *inner = call(
        second_kernel, [HALF, SQUARE, *INNER, *INNER], q, k, v, do, log_decay, b_sent,
        flops=100000000,
    )
    msg = call(message_kernel, [((CHIPS * MSG, 1, K), F32)], own, got, b)
    msg = exchanged(msg)
    back = call(scan_kernel, [SQUARE], msg)
    came = exchanged(back.reshape(CHIPS, ROWS, HK)).reshape(V, HK)
    onward, mine, *inner = call(
        onward_kernel,
        [SQUARE, SQUARE, *INNER, *INNER],
        own, got, b, came, q, k, v, do, b_sent, *inner,
        alias={9 + n: 2 + n for n in range(12)},
    )
    theirs = lax.ppermute(onward, "seq", SWAP)
    half = grads(True, (q, k, v, do, b, own, mine, *inner[:6]))
    return grads(False, (q, k, v, do, b_sent, send, theirs, *inner[6:]), half)


def solution(mesh):
    return jax.shard_map(
        local, mesh=mesh, in_specs=(SPEC,) * 5, out_specs=(SPEC,) * 4, check_vma=False
    )
```

```python
import jax
import jax.numpy as jnp
from jax import lax
from jax.experimental import pallas as pl
from jax.experimental.pallas import tpu as pltpu
from jax.sharding import PartitionSpec as P

H = 2
K = 128
V = 256
GROUP = 64
TOK = 256
HK = H * K
HV = H * V
Y, Z, CORES = 4, 8, 2
CHIPS = Y * Z
ROWS = V // CHIPS
MSG = 2 * ROWS + 1
SPEC = P(("batch", "seq"), None)
FIRST = (Y // 2, Z // 2)


def steps(chip):
    y, z = (chip // Z - FIRST[0]) % Y, (chip % Z - FIRST[1]) % Z
    return min(y, Y - y) + min(z, Z - z)


def steps_along_z(chip):
    z = (chip % Z - FIRST[1]) % Z
    return min(z, Z - z)


LISTED = sorted(range(CHIPS), key=lambda chip: (steps_along_z(chip), steps(chip)))
GROUPS = [[CORES * chip + core for chip in LISTED] for core in range(CORES)]
SWAP = [(device, device ^ 1) for device in range(CHIPS * CORES)]
F32 = jnp.float32
BF16 = jnp.bfloat16


def core_index():
    return lax.rem(lax.axis_index("seq"), CORES)


def exchanged(x):
    return lax.all_to_all(x, "seq", 0, 0, axis_index_groups=GROUPS, tiled=True)


def dot(left, right, dims):
    return lax.dot_general(left, right, (dims, ((), ())), preferred_element_type=F32)


def nn(left, right):
    return dot(left, right, ((1,), (0,)))


def nt(left, right):
    return dot(left, right, ((1,), (1,)))


def tn(left, right):
    return dot(left, right, ((0,), (0,)))


def split(x):
    hi = x.astype(BF16)
    return hi, (x - hi.astype(F32)).astype(BF16)


def pair(x):
    return jnp.concatenate(split(x), 1)


def folded(out):
    half = out.shape[1] // 2
    return out[:, :half] + out[:, half:]


def running_sum(x):
    rows = x.shape[0]
    r = lax.broadcasted_iota(jnp.int32, (rows, rows), 0)
    c = lax.broadcasted_iota(jnp.int32, (rows, rows), 1)
    ones = jnp.where(c <= r, 1.0, 0.0).astype(BF16)
    hi = x.astype(BF16)
    mid, lo = split(x - hi.astype(F32))
    return folded(nn(ones, halves(hi, mid))) + nn(ones, lo)


def head(h, width):
    return slice(h * width, (h + 1) * width)


def at_head(h, width):
    return pl.ds(pl.multiple_of(h * width, width), width)


def halves(left, right):
    return jnp.concatenate((left, right), 1)


def block_ends(q_ref, k_ref, v_ref, do_ref, b_ref, out_ref, h):
    hk, hv = at_head(h, K), at_head(h, V)
    b = b_ref[...]
    total = b_ref[TOK - 1 :]
    out_ref[:V, :K] = folded(tn(v_ref[:, hv], pair(k_ref[:, hk].astype(F32) * jnp.exp(total - b))))
    out_ref[:V, K:] = folded(tn(do_ref[:, hv], pair(q_ref[:, hk].astype(F32) * jnp.exp(b))))


def first_kernel(
    q_hbm, k_hbm, v_hbm, do_hbm, g_hbm, q_ref, k_ref, v_ref, do_ref, g_ref, b_ref, send_ref, sems
):
    core = core_index()
    pieces = ((g_hbm, g_ref, K), (k_hbm, k_ref, K), (v_hbm, v_ref, V), (q_hbm, q_ref, K), (do_hbm, do_ref, V))

    def copies(h, base):
        return [
            pltpu.make_async_copy(
                source.at[:, at_head(h, width)], target.at[:, at_head(h, width)], sems.at[base + n]
            )
            for n, (source, target, width) in enumerate(pieces)
        ]

    sent, kept = copies(1 - core, 0), copies(core, len(pieces))
    for copy in sent + kept:
        copy.start()
    sent[0].wait()
    b_ref[...] = running_sum(g_ref[:, at_head(1 - core, K)])
    for copy in sent[1:]:
        copy.wait()
    block_ends(q_ref, k_ref, v_ref, do_ref, b_ref, send_ref, 1 - core)
    total = b_ref[TOK - 1 :]
    send_ref[V:] = jnp.broadcast_to(halves(total, total), (8, HK))
    for copy in kept:
        copy.wait()


def inner_pairs(q_ref, k_ref, v_ref, do_ref, b_ref, h, dq_ref, dk_ref, dv_ref):
    hk, hv = at_head(h, K), at_head(h, V)
    r = lax.broadcasted_iota(jnp.int32, (TOK, TOK), 0)
    c = lax.broadcasted_iota(jnp.int32, (TOK, TOK), 1)
    q = q_ref[:, hk].astype(F32)
    k = k_ref[:, hk].astype(F32)
    b = b_ref[...]
    v = v_ref[:, hv]
    do = do_ref[:, hv]
    p_hi, p_lo = split(jnp.where(c <= r, nt(do, v), 0.0))
    t_hi, t_lo = split(jnp.where(c >= r, nt(v, do), 0.0))
    dk = jnp.zeros((TOK, K), F32)
    dv = jnp.zeros((TOK, V), F32)
    for i in range(TOK // GROUP):
        rows = slice(i * GROUP, (i + 1) * GROUP)
        end = (i + 1) * GROUP
        upto = slice(0, end)
        start = b[i * GROUP - 1 : i * GROUP] if i else jnp.zeros((1, K), F32)
        rising = jnp.exp(b[rows] - start)
        falling = jnp.exp(start - b[upto])
        q_hi, q_lo = split(q[rows] * rising)
        k_hi, k_lo = split(k[upto] * falling)
        scores_t = nt(k_hi, q_hi) + (nt(k_hi, q_lo) + nt(k_lo, q_hi))
        rr = lax.broadcasted_iota(jnp.int32, (end, GROUP), 0)
        cc = lax.broadcasted_iota(jnp.int32, (end, GROUP), 1) + i * GROUP
        s_hi, s_lo = split(jnp.where(cc >= rr, scores_t, 0.0))
        dq_ref[rows] = rising * (
            folded(nn(p_hi[rows, upto], halves(k_hi, k_lo))) + nn(p_lo[rows, upto], k_hi)
        )
        dk_part = falling * (
            folded(nn(t_hi[upto, rows], halves(q_hi, q_lo))) + nn(t_lo[upto, rows], q_hi)
        )
        dv_part = nn(s_hi, do[rows]) + nn(s_lo, do[rows])
        if end < TOK:
            dk_part = jnp.concatenate((dk_part, jnp.zeros((TOK - end, K), F32)), 0)
            dv_part = jnp.concatenate((dv_part, jnp.zeros((TOK - end, V), F32)), 0)
        dk = dk + dk_part
        dv = dv + dv_part
    dk_ref[...] = dk
    dv_ref[...] = dv


def outer_gates(k_ref, b_ref, h, rise_ref, tail_ref, kt_ref):
    b = b_ref[...]
    tail = jnp.exp(b_ref[TOK - 1 :] - b)
    rise_ref[...] = jnp.exp(b)
    tail_ref[...] = tail
    kt_ref[...] = pair(k_ref[:, at_head(h, K)].astype(F32) * tail)


def both_inner(q_ref, k_ref, v_ref, do_ref, b_ref, b_sent_ref, core, inner_refs):
    for h, sums_ref, refs in ((core, b_ref, inner_refs[:6]), (1 - core, b_sent_ref, inner_refs[6:])):
        inner_pairs(q_ref, k_ref, v_ref, do_ref, sums_ref, h, *refs[:3])
        outer_gates(k_ref, sums_ref, h, *refs[3:])


def second_kernel(q_ref, k_ref, v_ref, do_ref, g_ref, b_sent_ref, b_ref, own_ref, *inner_refs):
    core = core_index()
    b_ref[...] = running_sum(g_ref[:, at_head(core, K)])
    block_ends(q_ref, k_ref, v_ref, do_ref, b_ref, own_ref, core)

    @pl.when(core == 0)
    def _():
        both_inner(q_ref, k_ref, v_ref, do_ref, b_ref, b_sent_ref, core, inner_refs)


def lane_gates(b_ref, got_ref):
    core = core_index()
    total = b_ref[TOK - 1 :]
    mine = jnp.exp(halves(total, total))
    other = jnp.exp(got_ref[V : V + 1])
    forward = lax.broadcasted_iota(jnp.int32, (1, HK), 1) < K
    return mine, other, forward, core == 0


def pick(flag, forward, when_true, when_false):
    return jnp.where(jnp.logical_xor(forward, jnp.logical_not(flag)), when_true, when_false)


def message_kernel(own_ref, got_ref, b_ref, msg_ref):
    mine, other, forward, first = lane_gates(b_ref, got_ref)
    own_gate = pick(first, forward, other, 1.0)
    got_gate = pick(first, forward, 1.0, mine)
    for i in range(CHIPS):
        rows = slice(i * ROWS, (i + 1) * ROWS)
        chip = own_ref[rows] * own_gate + got_ref[rows] * got_gate
        for side in range(2):
            at = i * MSG + side * ROWS
            msg_ref[at : at + ROWS, 0, :] = chip[:, head(side, K)]
        msg_ref[i * MSG + 2 * ROWS] = (mine * other)[:, :K]


def scan_kernel(msg_ref, out_ref):
    places = [LISTED.index(chip) for chip in range(CHIPS)]
    for side, order in enumerate((places, places[::-1])):
        state = jnp.zeros((ROWS, K), F32)
        for i in order:
            out_ref[i * ROWS : (i + 1) * ROWS, head(side, K)] = state
            at = i * MSG + side * ROWS
            state = msg_ref[i * MSG + 2 * ROWS] * state + msg_ref[at : at + ROWS, 0, :]


def onward_kernel(
    own_ref, got_ref, b_ref, came_ref, q_ref, k_ref, v_ref, do_ref, b_sent_ref, *rest
):
    send_ref, mine_ref = rest[12:14]
    core = core_index()
    mine, other, forward, first = lane_gates(b_ref, got_ref)
    came = came_ref[...]
    send_ref[...] = came * pick(first, forward, mine, 1.0) + pick(
        first, forward, own_ref[...], 0.0
    )
    mine_ref[...] = came * pick(first, forward, 1.0, other) + pick(
        first, forward, 0.0, got_ref[:V]
    )

    @pl.when(core == 1)
    def _():
        both_inner(q_ref, k_ref, v_ref, do_ref, b_ref, b_sent_ref, core, rest[14:])


def head_grads(
    h, q_ref, k_ref, v_ref, do_ref, b_ref, end_ref, in_ref,
    dqi_ref, dki_ref, dvi_ref, rise_ref, tail_ref, kt_ref, dq_ref, dk_ref, dv_ref, dg_ref, stored,
):
    hk, hv = at_head(h, K), at_head(h, V)
    state = in_ref[:, :K]
    grad = in_ref[:, K:]
    g_hi, g_lo = split(grad)
    dv = dvi_ref[...] + (nt(kt_ref[...], halves(g_hi, g_hi)) + nt(kt_ref[:, :K], g_lo))
    dv_ref[...] = dv.astype(BF16)
    stored(2)
    dq = dqi_ref[...] + rise_ref[...] * folded(nn(do_ref[:, hv], pair(state)))
    dk = dki_ref[...] + tail_ref[...] * folded(nn(v_ref[:, hv], halves(g_hi, g_lo)))
    dq_ref[...] = dq.astype(BF16)
    stored(0)
    dk_ref[...] = dk.astype(BF16)
    stored(1)
    end_state = jnp.exp(b_ref[TOK - 1 :]) * state + end_ref[:V, :K]
    later = jnp.sum(end_state * grad, axis=0, keepdims=True)
    terms = q_ref[:, hk].astype(F32) * dq - k_ref[:, hk].astype(F32) * dk
    r = lax.broadcasted_iota(jnp.int32, (TOK, TOK), 0)
    c = lax.broadcasted_iota(jnp.int32, (TOK, TOK), 1)
    ones = jnp.where(c >= r, 1.0, 0.0).astype(BF16)
    dg_ref[...] = folded(nn(ones, pair(terms))) + later
    stored(3)


def grads_kernel(own, q_ref, k_ref, v_ref, do_ref, b_ref, end_ref, in_ref, *rest):
    inner_refs, outs, halves_out, sems = rest[:6], rest[-9:-5], rest[-5:-1], rest[-1]
    core = core_index()
    h = core if own else 1 - core
    copies = [
        pltpu.make_async_copy(source, out.at[:, at_head(h, width)], sems.at[n])
        for n, (source, out, width) in enumerate(zip(halves_out, outs, (K, K, V, K)))
    ]
    head_grads(
        h, q_ref, k_ref, v_ref, do_ref, b_ref, end_ref, in_ref, *inner_refs, *halves_out,
        lambda n: copies[n].start(),
    )
    for copy in copies:
        copy.wait()


VMEM = pl.BlockSpec(memory_space=pltpu.VMEM)
HBM = pl.BlockSpec(memory_space=pltpu.HBM)
SQUARE = ((TOK, HK), F32)
SQUARE16 = ((TOK, HK), BF16)
WIDE16 = ((TOK, HV), BF16)
HALF = ((TOK, K), F32)
INNER = [HALF, HALF, ((TOK, V), F32), HALF, HALF, ((TOK, 2 * K), BF16)]
HALF_GRADS = [((TOK, K), BF16), ((TOK, K), BF16), ((TOK, V), BF16), HALF]


def call(kernel, outs, *args, specs=None, out_specs=None, scratch=(), flops=1000000, alias=None):
    shapes = [jax.ShapeDtypeStruct(shape, dtype) for shape, dtype in outs]
    out = pl.pallas_call(
        kernel,
        out_shape=shapes,
        in_specs=specs or [VMEM] * len(args),
        out_specs=out_specs or [VMEM] * len(outs),
        scratch_shapes=list(scratch),
        input_output_aliases=alias or {},
        cost_estimate=pl.CostEstimate(flops=flops, bytes_accessed=2000000, transcendentals=0),
        compiler_params=pltpu.CompilerParams(vmem_limit_bytes=32 << 20),
    )(*args)
    return out if len(outs) > 1 else out[0]


def grads(own, args, into=()):
    def kernel(*refs):
        grads_kernel(own, *refs)

    return call(
        kernel,
        [SQUARE16, SQUARE16, WIDE16, SQUARE],
        *args,
        *into,
        specs=[VMEM] * len(args) + [HBM] * len(into),
        out_specs=[HBM] * 4,
        scratch=[pltpu.VMEM(*out) for out in HALF_GRADS] + [pltpu.SemaphoreType.DMA((4,))],
        flops=100000000,
        alias={len(args) + n: n for n in range(len(into))},
    )


def local(q, k, v, log_decay, do):
    q, k, v, do, log_decay = (
        pltpu.with_memory_space_constraint(x, pltpu.HBM) for x in (q, k, v, do, log_decay)
    )
    q, k, v, do, log_decay, b_sent, send = call(
        first_kernel,
        [SQUARE16, SQUARE16, WIDE16, WIDE16, SQUARE, HALF, ((V + 8, HK), F32)],
        q, k, v, do, log_decay,
        specs=[HBM] * 5,
        scratch=[pltpu.SemaphoreType.DMA((10,))],
    )
    got = lax.ppermute(send, "seq", SWAP)
    b, own, *inner = call(
        second_kernel, [HALF, SQUARE, *INNER, *INNER], q, k, v, do, log_decay, b_sent,
        flops=100000000,
    )
    msg = call(message_kernel, [((CHIPS * MSG, 1, K), F32)], own, got, b)
    msg = exchanged(msg)
    back = call(scan_kernel, [SQUARE], msg)
    came = exchanged(back.reshape(CHIPS, ROWS, HK)).reshape(V, HK)
    onward, mine, *inner = call(
        onward_kernel,
        [SQUARE, SQUARE, *INNER, *INNER],
        own, got, b, came, q, k, v, do, b_sent, *inner,
        alias={9 + n: 2 + n for n in range(12)},
    )
    theirs = lax.ppermute(onward, "seq", SWAP)
    half = grads(True, (q, k, v, do, b, own, mine, *inner[:6]))
    return grads(False, (q, k, v, do, b_sent, send, theirs, *inner[6:]), half)


def solution(mesh):
    return jax.shard_map(
        local, mesh=mesh, in_specs=(SPEC,) * 5, out_specs=(SPEC,) * 4, check_vma=False
    )
```

```python
import jax
import jax.numpy as jnp
from jax import lax
from jax.experimental import pallas as pl
from jax.experimental.pallas import tpu as pltpu
from jax.sharding import PartitionSpec as P

H = 2
K = 128
V = 256
GROUP = 64
TOK = 256
HK = H * K
HV = H * V
Y, Z, CORES = 4, 8, 2
CHIPS = Y * Z
ROWS = V // CHIPS
MSG = 2 * ROWS + 1
SPEC = P(("batch", "seq"), None)
FIRST = (Y // 2, Z // 2)


def steps(chip):
    y, z = (chip // Z - FIRST[0]) % Y, (chip % Z - FIRST[1]) % Z
    return min(y, Y - y) + min(z, Z - z)


LISTED = sorted(range(CHIPS), key=steps)
GROUPS = [[CORES * chip + core for chip in LISTED] for core in range(CORES)]
SWAP = [(device, device ^ 1) for device in range(CHIPS * CORES)]
F32 = jnp.float32
BF16 = jnp.bfloat16


def core_index():
    return lax.rem(lax.axis_index("seq"), CORES)


def exchanged(x):
    return lax.all_to_all(x, "seq", 0, 0, axis_index_groups=GROUPS, tiled=True)


def dot(left, right, dims):
    return lax.dot_general(left, right, (dims, ((), ())), preferred_element_type=F32)


def nn(left, right):
    return dot(left, right, ((1,), (0,)))


def nt(left, right):
    return dot(left, right, ((1,), (1,)))


def tn(left, right):
    return dot(left, right, ((0,), (0,)))


def split(x):
    hi = x.astype(BF16)
    return hi, (x - hi.astype(F32)).astype(BF16)


def pair(x):
    return jnp.concatenate(split(x), 1)


def folded(out):
    half = out.shape[1] // 2
    return out[:, :half] + out[:, half:]


def running_sum(x):
    rows = x.shape[0]
    r = lax.broadcasted_iota(jnp.int32, (rows, rows), 0)
    c = lax.broadcasted_iota(jnp.int32, (rows, rows), 1)
    ones = jnp.where(c <= r, 1.0, 0.0).astype(BF16)
    hi = x.astype(BF16)
    mid, lo = split(x - hi.astype(F32))
    return folded(nn(ones, halves(hi, mid))) + nn(ones, lo)


def head(h, width):
    return slice(h * width, (h + 1) * width)


def at_head(h, width):
    return pl.ds(pl.multiple_of(h * width, width), width)


def halves(left, right):
    return jnp.concatenate((left, right), 1)


def block_ends(q_ref, k_ref, v_ref, do_ref, b_ref, out_ref, h):
    hk, hv = at_head(h, K), at_head(h, V)
    b = b_ref[...]
    total = b_ref[TOK - 1 :]
    out_ref[:V, :K] = folded(tn(v_ref[:, hv], pair(k_ref[:, hk].astype(F32) * jnp.exp(total - b))))
    out_ref[:V, K:] = folded(tn(do_ref[:, hv], pair(q_ref[:, hk].astype(F32) * jnp.exp(b))))


def first_kernel(
    q_hbm, k_hbm, v_hbm, do_hbm, g_hbm, q_ref, k_ref, v_ref, do_ref, g_ref, b_ref, send_ref, sems
):
    core = core_index()
    pieces = ((g_hbm, g_ref, K), (k_hbm, k_ref, K), (v_hbm, v_ref, V), (q_hbm, q_ref, K), (do_hbm, do_ref, V))

    def copies(h, base):
        return [
            pltpu.make_async_copy(
                source.at[:, at_head(h, width)], target.at[:, at_head(h, width)], sems.at[base + n]
            )
            for n, (source, target, width) in enumerate(pieces)
        ]

    sent, kept = copies(1 - core, 0), copies(core, len(pieces))
    for copy in sent:
        copy.start()
    for copy in kept:
        copy.start(priority=1)
    sent[0].wait()
    b_ref[...] = running_sum(g_ref[:, at_head(1 - core, K)])
    for copy in sent[1:]:
        copy.wait()
    block_ends(q_ref, k_ref, v_ref, do_ref, b_ref, send_ref, 1 - core)
    total = b_ref[TOK - 1 :]
    send_ref[V:] = jnp.broadcast_to(halves(total, total), (8, HK))
    for copy in kept:
        copy.wait()


def inner_pairs(q_ref, k_ref, v_ref, do_ref, b_ref, h, dq_ref, dk_ref, dv_ref):
    hk, hv = at_head(h, K), at_head(h, V)
    r = lax.broadcasted_iota(jnp.int32, (TOK, TOK), 0)
    c = lax.broadcasted_iota(jnp.int32, (TOK, TOK), 1)
    q = q_ref[:, hk].astype(F32)
    k = k_ref[:, hk].astype(F32)
    b = b_ref[...]
    v = v_ref[:, hv]
    do = do_ref[:, hv]
    p_hi, p_lo = split(jnp.where(c <= r, nt(do, v), 0.0))
    t_hi, t_lo = split(jnp.where(c >= r, nt(v, do), 0.0))
    dk = jnp.zeros((TOK, K), F32)
    dv = jnp.zeros((TOK, V), F32)
    for i in range(TOK // GROUP):
        rows = slice(i * GROUP, (i + 1) * GROUP)
        end = (i + 1) * GROUP
        upto = slice(0, end)
        start = b[i * GROUP - 1 : i * GROUP] if i else jnp.zeros((1, K), F32)
        rising = jnp.exp(b[rows] - start)
        falling = jnp.exp(start - b[upto])
        q_hi, q_lo = split(q[rows] * rising)
        k_hi, k_lo = split(k[upto] * falling)
        scores_t = nt(k_hi, q_hi) + (nt(k_hi, q_lo) + nt(k_lo, q_hi))
        rr = lax.broadcasted_iota(jnp.int32, (end, GROUP), 0)
        cc = lax.broadcasted_iota(jnp.int32, (end, GROUP), 1) + i * GROUP
        s_hi, s_lo = split(jnp.where(cc >= rr, scores_t, 0.0))
        dq_ref[rows] = rising * (
            folded(nn(p_hi[rows, upto], halves(k_hi, k_lo))) + nn(p_lo[rows, upto], k_hi)
        )
        dk_part = falling * (
            folded(nn(t_hi[upto, rows], halves(q_hi, q_lo))) + nn(t_lo[upto, rows], q_hi)
        )
        dv_part = nn(s_hi, do[rows]) + nn(s_lo, do[rows])
        if end < TOK:
            dk_part = jnp.concatenate((dk_part, jnp.zeros((TOK - end, K), F32)), 0)
            dv_part = jnp.concatenate((dv_part, jnp.zeros((TOK - end, V), F32)), 0)
        dk = dk + dk_part
        dv = dv + dv_part
    dk_ref[...] = dk
    dv_ref[...] = dv


def outer_gates(k_ref, b_ref, h, rise_ref, tail_ref, kt_ref):
    b = b_ref[...]
    tail = jnp.exp(b_ref[TOK - 1 :] - b)
    rise_ref[...] = jnp.exp(b)
    tail_ref[...] = tail
    kt_ref[...] = pair(k_ref[:, at_head(h, K)].astype(F32) * tail)


def both_inner(q_ref, k_ref, v_ref, do_ref, b_ref, b_sent_ref, core, inner_refs):
    for h, sums_ref, refs in ((core, b_ref, inner_refs[:6]), (1 - core, b_sent_ref, inner_refs[6:])):
        inner_pairs(q_ref, k_ref, v_ref, do_ref, sums_ref, h, *refs[:3])
        outer_gates(k_ref, sums_ref, h, *refs[3:])


def second_kernel(q_ref, k_ref, v_ref, do_ref, g_ref, b_sent_ref, b_ref, own_ref, *inner_refs):
    core = core_index()
    b_ref[...] = running_sum(g_ref[:, at_head(core, K)])
    block_ends(q_ref, k_ref, v_ref, do_ref, b_ref, own_ref, core)

    @pl.when(core == 0)
    def _():
        both_inner(q_ref, k_ref, v_ref, do_ref, b_ref, b_sent_ref, core, inner_refs)


def lane_gates(b_ref, got_ref):
    core = core_index()
    total = b_ref[TOK - 1 :]
    mine = jnp.exp(halves(total, total))
    other = jnp.exp(got_ref[V : V + 1])
    forward = lax.broadcasted_iota(jnp.int32, (1, HK), 1) < K
    return mine, other, forward, core == 0


def pick(flag, forward, when_true, when_false):
    return jnp.where(jnp.logical_xor(forward, jnp.logical_not(flag)), when_true, when_false)


def message_kernel(own_ref, got_ref, b_ref, msg_ref):
    mine, other, forward, first = lane_gates(b_ref, got_ref)
    own_gate = pick(first, forward, other, 1.0)
    got_gate = pick(first, forward, 1.0, mine)
    for i in range(CHIPS):
        rows = slice(i * ROWS, (i + 1) * ROWS)
        chip = own_ref[rows] * own_gate + got_ref[rows] * got_gate
        for side in range(2):
            at = i * MSG + side * ROWS
            msg_ref[at : at + ROWS, 0, :] = chip[:, head(side, K)]
        msg_ref[i * MSG + 2 * ROWS] = (mine * other)[:, :K]


def scan_kernel(msg_ref, out_ref):
    places = [LISTED.index(chip) for chip in range(CHIPS)]
    for side, order in enumerate((places, places[::-1])):
        state = jnp.zeros((ROWS, K), F32)
        for i in order:
            out_ref[i * ROWS : (i + 1) * ROWS, head(side, K)] = state
            at = i * MSG + side * ROWS
            state = msg_ref[i * MSG + 2 * ROWS] * state + msg_ref[at : at + ROWS, 0, :]


def onward_kernel(
    own_ref, got_ref, b_ref, came_ref, q_ref, k_ref, v_ref, do_ref, b_sent_ref, *rest
):
    send_ref, mine_ref = rest[12:14]
    core = core_index()
    mine, other, forward, first = lane_gates(b_ref, got_ref)
    came = came_ref[...]
    send_ref[...] = came * pick(first, forward, mine, 1.0) + pick(
        first, forward, own_ref[...], 0.0
    )
    mine_ref[...] = came * pick(first, forward, 1.0, other) + pick(
        first, forward, 0.0, got_ref[:V]
    )

    @pl.when(core == 1)
    def _():
        both_inner(q_ref, k_ref, v_ref, do_ref, b_ref, b_sent_ref, core, rest[14:])


def head_grads(
    h, q_ref, k_ref, v_ref, do_ref, b_ref, end_ref, in_ref,
    dqi_ref, dki_ref, dvi_ref, rise_ref, tail_ref, kt_ref, dq_ref, dk_ref, dv_ref, dg_ref, stored,
):
    hk, hv = at_head(h, K), at_head(h, V)
    state = in_ref[:, :K]
    grad = in_ref[:, K:]
    g_hi, g_lo = split(grad)
    dq = dqi_ref[...] + rise_ref[...] * folded(nn(do_ref[:, hv], pair(state)))
    dk = dki_ref[...] + tail_ref[...] * folded(nn(v_ref[:, hv], halves(g_hi, g_lo)))
    dq_ref[...] = dq.astype(BF16)
    stored(0)
    dk_ref[...] = dk.astype(BF16)
    stored(1)
    dv = dvi_ref[...] + (nt(kt_ref[...], halves(g_hi, g_hi)) + nt(kt_ref[:, :K], g_lo))
    dv_ref[...] = dv.astype(BF16)
    stored(2)
    end_state = jnp.exp(b_ref[TOK - 1 :]) * state + end_ref[:V, :K]
    later = jnp.sum(end_state * grad, axis=0, keepdims=True)
    terms = q_ref[:, hk].astype(F32) * dq - k_ref[:, hk].astype(F32) * dk
    r = lax.broadcasted_iota(jnp.int32, (TOK, TOK), 0)
    c = lax.broadcasted_iota(jnp.int32, (TOK, TOK), 1)
    ones = jnp.where(c >= r, 1.0, 0.0).astype(BF16)
    dg_ref[...] = folded(nn(ones, pair(terms))) + later
    stored(3)


def grads_kernel(own, q_ref, k_ref, v_ref, do_ref, b_ref, end_ref, in_ref, *rest):
    inner_refs, outs, halves_out, sems = rest[:6], rest[-9:-5], rest[-5:-1], rest[-1]
    core = core_index()
    h = core if own else 1 - core
    copies = [
        pltpu.make_async_copy(source, out.at[:, at_head(h, width)], sems.at[n])
        for n, (source, out, width) in enumerate(zip(halves_out, outs, (K, K, V, K)))
    ]
    head_grads(
        h, q_ref, k_ref, v_ref, do_ref, b_ref, end_ref, in_ref, *inner_refs, *halves_out,
        lambda n: copies[n].start(),
    )
    for copy in copies:
        copy.wait()


VMEM = pl.BlockSpec(memory_space=pltpu.VMEM)
HBM = pl.BlockSpec(memory_space=pltpu.HBM)
SQUARE = ((TOK, HK), F32)
SQUARE16 = ((TOK, HK), BF16)
WIDE16 = ((TOK, HV), BF16)
HALF = ((TOK, K), F32)
INNER = [HALF, HALF, ((TOK, V), F32), HALF, HALF, ((TOK, 2 * K), BF16)]
HALF_GRADS = [((TOK, K), BF16), ((TOK, K), BF16), ((TOK, V), BF16), HALF]


def call(kernel, outs, *args, specs=None, out_specs=None, scratch=(), flops=1000000, alias=None):
    shapes = [jax.ShapeDtypeStruct(shape, dtype) for shape, dtype in outs]
    out = pl.pallas_call(
        kernel,
        out_shape=shapes,
        in_specs=specs or [VMEM] * len(args),
        out_specs=out_specs or [VMEM] * len(outs),
        scratch_shapes=list(scratch),
        input_output_aliases=alias or {},
        cost_estimate=pl.CostEstimate(flops=flops, bytes_accessed=2000000, transcendentals=0),
        compiler_params=pltpu.CompilerParams(vmem_limit_bytes=32 << 20),
    )(*args)
    return out if len(outs) > 1 else out[0]


def grads(own, args, into=()):
    def kernel(*refs):
        grads_kernel(own, *refs)

    return call(
        kernel,
        [SQUARE16, SQUARE16, WIDE16, SQUARE],
        *args,
        *into,
        specs=[VMEM] * len(args) + [HBM] * len(into),
        out_specs=[HBM] * 4,
        scratch=[pltpu.VMEM(*out) for out in HALF_GRADS] + [pltpu.SemaphoreType.DMA((4,))],
        flops=100000000,
        alias={len(args) + n: n for n in range(len(into))},
    )


def local(q, k, v, log_decay, do):
    q, k, v, do, log_decay = (
        pltpu.with_memory_space_constraint(x, pltpu.HBM) for x in (q, k, v, do, log_decay)
    )
    q, k, v, do, log_decay, b_sent, send = call(
        first_kernel,
        [SQUARE16, SQUARE16, WIDE16, WIDE16, SQUARE, HALF, ((V + 8, HK), F32)],
        q, k, v, do, log_decay,
        specs=[HBM] * 5,
        scratch=[pltpu.SemaphoreType.DMA((10,))],
    )
    got = lax.ppermute(send, "seq", SWAP)
    b, own, *inner = call(
        second_kernel, [HALF, SQUARE, *INNER, *INNER], q, k, v, do, log_decay, b_sent,
        flops=100000000,
    )
    msg = call(message_kernel, [((CHIPS * MSG, 1, K), F32)], own, got, b)
    msg = exchanged(msg)
    back = call(scan_kernel, [SQUARE], msg)
    came = exchanged(back.reshape(CHIPS, ROWS, HK)).reshape(V, HK)
    onward, mine, *inner = call(
        onward_kernel,
        [SQUARE, SQUARE, *INNER, *INNER],
        own, got, b, came, q, k, v, do, b_sent, *inner,
        alias={9 + n: 2 + n for n in range(12)},
    )
    theirs = lax.ppermute(onward, "seq", SWAP)
    half = grads(True, (q, k, v, do, b, own, mine, *inner[:6]))
    return grads(False, (q, k, v, do, b_sent, send, theirs, *inner[6:]), half)


def solution(mesh):
    return jax.shard_map(
        local, mesh=mesh, in_specs=(SPEC,) * 5, out_specs=(SPEC,) * 4, check_vma=False
    )
```
